256 devices in a mesh: dp: 8 (over z), table: 32 (over y, x, core).
Axes of the slice: x: 4, y: 4, z: 8, core: 2. Of those that a mesh axis runs over, the one named last changes fastest.
Arguments:
- queries: bfloat16 [32768, 2, 512], P(('dp', 'table')), may hold values from -6 to 6
- sub_keys: bfloat16 [2, 2, 512, 256], replicated, may hold values from -0.375 to 0.375
- values: bfloat16 [512, 512, 1024], P('table', None, 'dp'), may hold values from -0.1875 to 0.1875
- slot_first: int32 [32768, 2, 4], P(('dp', 'table')), may hold values from 0 to 511, as said below
- slot_second: int32 [32768, 2, 4], P(('dp', 'table')), may hold values from 0 to 511
- cotangent: bfloat16 [32768, 1024], P(('dp', 'table')), may hold values from -6 to 6
Outputs:
- value_update: float32 [512, 512, 1024], P('table', None, 'dp')
- key_update: float32 [2, 2, 512, 256], P(None, None, ('dp', 'table'))
- clip_factor: float32 [1], replicated
The draws below stay inside these ranges and needn't reach their ends.
Inputs may be any that keep to these rules, and one draw needn't show every extreme that they name: Within each aligned block of 128 tokens (the tokens of one device), at most 48 of its 1024 slots have slot_first in any one range [r * 16, (r + 1) * 16), and exactly 48 do in one such range.
All inputs are finite; a program needn't handle non-finite values.
Results may differ from the reference program's by a relative error of at most 0.0003.
Values may be sent and summed in bfloat16 or wider, within the bound.
No kernel may reach another device: no remote copies, remote signals or barrier semaphores. Data moves between devices by JAX's collectives and lax.ppermute only.
A program may use at most 64 MiB of HBM per device.

```python
import math
import jax
import jax.numpy as jnp
from jax import lax

NSUB = 512
DV = 1024
DK = 512
HEADS = 2
KTOP = 4
TOK_DEV = 128
HALF_DK = 256
TOKENS = 32768
BLK = 16
CAP = 48
N_TABLE = 32


def draw_slot_first(key, part):
    slot_count = TOK_DEV * HEADS * KTOP
    block_count = TOKENS // TOK_DEV
    ranking = jax.random.permutation(jax.random.fold_in(key, 3), N_TABLE)
    choices_hot = max(1, N_TABLE // 8)

    def one_block(block_key):
        subkeys = jax.random.split(block_key, 3)
        busiest = ranking[jax.random.randint(subkeys[0], (), 0, choices_hot)]
        positions = jnp.arange(slot_count, dtype=jnp.int32)
        spread_index = (positions - CAP) % (N_TABLE - 1)
        owners = jnp.where(positions < CAP, busiest, (busiest + 1 + spread_index) % N_TABLE)
        owners = jax.random.permutation(subkeys[1], owners)
        offsets = jax.random.randint(subkeys[2], (slot_count,), 0, BLK)
        return (owners * BLK + offsets).reshape(TOK_DEV, HEADS, KTOP)
    blocks = jax.vmap(one_block)(jax.random.split(jax.random.fold_in(key, 7), block_count))
    return blocks.reshape(TOKENS, HEADS, KTOP).astype(jnp.int32)


def place_ends(values, own_key, smallest, high):
    dims = values.shape
    index_at = [jax.random.randint(jax.random.fold_in(own_key, axis), (), 0, dims[axis]) for axis in range(len(dims))]
    values = values.at[tuple(index_at)].set(smallest)
    longest = dims.index(max(dims))
    index_at[longest] = (index_at[longest] + 1) % dims[longest]
    return values.at[tuple(index_at)].set(high)


def levels(rng, dims, cuts, low, top_value):
    level = 1.0
    for position, blocks in cuts:
        draws = jax.random.uniform(jax.random.fold_in(jax.random.fold_in(rng, 6), position), (blocks,), jnp.float32, low / len(cuts), top_value / len(cuts))
        level = level * jnp.repeat(jnp.exp(draws), dims[position] // blocks).reshape((-1,) + (1,) * (len(dims) - 1 - position))
    return level


def scatter_about(rng, dims, scale, most, pieces=(), kind=jnp.bfloat16):
    array = jax.random.normal(rng, dims, jnp.float32) * scale
    if len(pieces) > 0:
        array = levels(rng, dims, pieces, -0.22, 0.18) * array
    return jnp.clip(array, min=-most, max=most).astype(kind)


def setup_inputs(seed: int = 0) -> dict:
    keys = jax.random.split(jax.random.key(seed), 7)
    return {
        "queries": scatter_about(keys[0], (TOKENS, HEADS, DK), 1.0, 6.0, ((0, 256),)),
        "sub_keys": scatter_about(keys[1], (2, HEADS, NSUB, HALF_DK), HALF_DK ** -0.5, 0.375),
        "values": scatter_about(keys[2], (NSUB, NSUB, DV), DV ** -0.5, 0.1875, ((0, 32), (2, 8))),
        "slot_first": draw_slot_first(jax.random.fold_in(keys[6], 71), 0),
        "slot_second": place_ends(jax.random.randint(keys[4], (TOKENS, HEADS, KTOP), 0, NSUB), jax.random.fold_in(keys[4], 1), 0, NSUB - 1).astype(jnp.int32),
        "cotangent": scatter_about(keys[5], (TOKENS, DV), 1.0, 6.0, ((0, 256),)),
    }


limit_ratio = 5.0

def reference(queries, sub_keys, values, slot_first, slot_second, cotangent):
    half_width = DK // 2
    table_rows = values.reshape(NSUB * NSUB, DV)
    head_ids = jnp.arange(HEADS, dtype=jnp.int32)[None, :, None]
    block_count = TOKENS // TOK_DEV
    highest = lax.Precision.HIGHEST

    def visit_block(carry, records):
        value_grad, key_grad = carry
        query_block, first_block, second_block, grad_block = records
        query_first = query_block[:, :, :half_width].astype(jnp.float32)
        query_second = query_block[:, :, half_width:].astype(jnp.float32)
        key_first = sub_keys[0][head_ids, first_block].astype(jnp.float32)
        key_second = sub_keys[1][head_ids, second_block].astype(jnp.float32)
        raw_score = jnp.einsum('thc,thkc->thk', query_first, key_first, precision=highest)
        raw_score = raw_score + jnp.einsum('thc,thkc->thk', query_second, key_second, precision=highest)
        exp_score = jnp.exp(raw_score)
        weight = exp_score / lax.optimization_barrier(jnp.sum(exp_score, axis=2, keepdims=True))
        row_index = (first_block * NSUB + second_block).astype(jnp.int32)
        grad_wide = grad_block.astype(jnp.float32)
        picked_rows = table_rows[row_index].astype(jnp.float32)
        picked = jnp.einsum('tc,thkc->thk', grad_wide, picked_rows, precision=highest)
        dscore = weight * (picked - lax.optimization_barrier(jnp.sum(weight * picked, axis=2, keepdims=True)))
        updates = weight[:, :, :, None] * grad_wide[:, None, None, :]
        value_grad = value_grad.at[row_index.reshape(-1)].add(updates.reshape(-1, DV))
        labels_first = (head_ids * NSUB + first_block).reshape(-1)
        labels_second = (head_ids * NSUB + second_block).reshape(-1)
        terms_first = (dscore[:, :, :, None] * query_first[:, :, None, :]).reshape(-1, half_width)
        terms_second = (dscore[:, :, :, None] * query_second[:, :, None, :]).reshape(-1, half_width)
        sums_first = jax.ops.segment_sum(terms_first, labels_first, num_segments=HEADS * NSUB)
        sums_second = jax.ops.segment_sum(terms_second, labels_second, num_segments=HEADS * NSUB)
        key_grad = key_grad + jnp.stack([sums_first, sums_second]).reshape(2, HEADS, NSUB, half_width)
        return ((value_grad, key_grad), None)
    records = (queries.reshape(block_count, TOK_DEV, HEADS, DK), slot_first.reshape(block_count, TOK_DEV, HEADS, KTOP), slot_second.reshape(block_count, TOK_DEV, HEADS, KTOP), cotangent.reshape(block_count, TOK_DEV, DV))
    start = (jnp.zeros((NSUB * NSUB, DV), jnp.float32), jnp.zeros((2, HEADS, NSUB, half_width), jnp.float32))
    (value_grad, key_grad), _ = lax.scan(visit_block, start, records)
    total_sq = jnp.sum(value_grad * value_grad) + jnp.sum(key_grad * key_grad)
    clip_factor = jnp.minimum(1.0, limit_ratio * math.sqrt(TOKENS) / jnp.sqrt(total_sq))
    value_update = (clip_factor * value_grad).reshape(NSUB, NSUB, DV)
    key_update = clip_factor * key_grad
    return (value_update, key_update, clip_factor.reshape(1))
```

```python
import math

import jax
import jax.numpy as jnp
from jax import lax
from jax.experimental import pallas as pl
from jax.experimental.pallas import tpu as pltpu
from jax.sharding import Mesh
from jax.sharding import PartitionSpec as P

TABLE = ("table_0", "table_1", "table_2")
DP_TABLE = ("dp", "table_0", "table_1", "table_2")
ALL = ("dp", "table_0", "table_1", "table_2")
NSUB = 512
BLK = 16
CAP = 48
OWN = 32
NDP = 8
TOK = 128
PICKS = 8
HALF = 256
KEYS = NSUB // NDP
LISTS = OWN * NDP
ROWS = BLK * NSUB
ACCS = 4
F32 = jnp.float32
BF16 = jnp.bfloat16
LIMIT_RATIO = 5.0

NT = (((1,), (1,)), ((), ()))
NN = (((1,), (0,)), ((), ()))


def pieces(x):
    high = x.astype(BF16)
    rest = x - high.astype(F32)
    mid = rest.astype(BF16)
    low = (rest - mid.astype(F32)).astype(BF16)
    return high, mid, low


def prep_kernel(q_ref, keys_ref, first_ref, second_ref, rec_ref, aux_ref):
    first = first_ref[...]
    second = second_ref[...]
    key_id = lax.broadcasted_iota(jnp.int32, (NSUB, TOK), 0)
    scores = [None] * PICKS
    for half, index in ((0, first), (1, second)):
        for head in range(2):
            at = head * 2 * HALF + half * HALF
            table = lax.dot_general(
                keys_ref[half, head], q_ref[:, at : at + HALF], NT, preferred_element_type=F32
            )
            for k in range(4):
                slot = head * 4 + k
                part = jnp.sum(
                    jnp.where(key_id == index[slot : slot + 1, :], table, 0.0),
                    axis=0,
                    keepdims=True,
                )
                scores[slot] = part if scores[slot] is None else scores[slot] + part
    exps = [jnp.exp(s) for s in scores]
    weights = []
    for head in range(2):
        e = exps[head * 4 : head * 4 + 4]
        total = (e[0] + e[1]) + (e[2] + e[3])
        weights += [x / total for x in e]
    owner = jnp.right_shift(first, 4)
    owner_id = lax.broadcasted_iota(jnp.int32, (OWN, TOK), 0)
    member = [
        jnp.where(owner_id == owner[s : s + 1, :], 1.0, 0.0).astype(F32) for s in range(PICKS)
    ]
    earlier = jnp.where(
        lax.broadcasted_iota(jnp.int32, (TOK, TOK), 0)
        < lax.broadcasted_iota(jnp.int32, (TOK, TOK), 1),
        1.0,
        0.0,
    ).astype(BF16)
    member_all = jnp.concatenate(member, axis=0).astype(BF16)
    ranks = lax.dot_general(member_all, earlier, NN, preferred_element_type=F32)
    base = jnp.zeros((OWN, 1), F32)
    token = lax.broadcasted_iota(jnp.int32, (1, TOK), 1)
    lane_id = lax.broadcasted_iota(jnp.int32, (TOK, TOK), 0)
    record = jnp.zeros((OWN, TOK), F32)
    targets = []
    for s in range(PICKS):
        rank = jnp.sum(
            member[s] * (ranks[s * OWN : (s + 1) * OWN, :] + base), axis=0, keepdims=True
        )
        base = base + jnp.sum(member[s], axis=1, keepdims=True)
        place = rank.astype(jnp.int32)
        code = (
            (jnp.bitwise_and(first[s : s + 1, :], BLK - 1) * NSUB + second[s : s + 1, :]) * TOK
            + token
        ).astype(F32)
        entry = jnp.where(lane_id == place, code, 0.0) + jnp.where(
            lane_id == place + CAP, weights[s], 0.0
        )
        for piece in pieces(entry):
            record = record + lax.dot_general(
                member[s].astype(BF16), piece, NT, preferred_element_type=F32
            )
        targets.append((owner[s : s + 1, :] * TOK + place).astype(F32))
    lane = lax.broadcasted_iota(jnp.int32, (OWN, TOK), 1)
    rec_ref[...] = jnp.where(lane == 2 * CAP, base, record)
    aux_ref[0:8, :] = jnp.concatenate(weights, axis=0)
    aux_ref[8:16, :] = jnp.concatenate(targets, axis=0)
    aux_ref[16:24, :] = first.astype(F32)
    aux_ref[24:32, :] = second.astype(F32)


def prep(q, keys, first, second):
    return pl.pallas_call(
        prep_kernel,
        out_shape=(
            jax.ShapeDtypeStruct((OWN, TOK), F32),
            jax.ShapeDtypeStruct((32, TOK), F32),
        ),
        name="prep",
    )(q, keys, first, second)


def expand_kernel(rec_ref, cot_ref, out_ref):
    record = rec_ref[0]
    square = jnp.concatenate([record, record, record, record], axis=0)
    columns = jnp.transpose(square)
    token = jnp.bitwise_and(columns[0:CAP, :].astype(jnp.int32), TOK - 1)
    lane = lax.broadcasted_iota(jnp.int32, (CAP, TOK), 1)
    cot = cot_ref[0]
    for o in range(OWN):
        chosen = jnp.where(token[:, o : o + 1] == lane, 1.0, 0.0).astype(BF16)
        out_ref[o, 0] = lax.dot_general(
            chosen, cot, NN, preferred_element_type=F32
        ).astype(BF16)


def expand(records, cot):
    return pl.pallas_call(
        expand_kernel,
        grid=(NDP,),
        in_specs=[
            pl.BlockSpec((1, OWN, TOK), lambda s: (s, 0, 0)),
            pl.BlockSpec((1, TOK, TOK), lambda s: (s, 0, 0)),
        ],
        out_specs=pl.BlockSpec((OWN, 1, CAP, TOK), lambda s: (0, s, 0, 0)),
        out_shape=jax.ShapeDtypeStruct((OWN, NDP, CAP, TOK), BF16),
        name="expand",
    )(records, cot)


GATHER_LISTS = 16


def gather_kernel(row_ref, table_ref, out_ref, wide_ref, got_ref):
    step = pl.program_id(0)

    @pl.when(step == 0)
    def _():
        def widen(i, carry):
            at = pl.multiple_of(i * 256, 256)
            wide_ref[pl.ds(at, 256), :] = table_ref[pl.ds(at, 256), :].astype(F32)
            return carry

        lax.fori_loop(0, ROWS // 256, widen, 0)

    def one_list(i, carry):
        for j in range(CAP):
            row = row_ref[step * GATHER_LISTS + i, j]
            got_ref[pl.ds(i * CAP + j, 1), :] = wide_ref[pl.ds(row, 1), :]
        return carry

    lax.fori_loop(0, GATHER_LISTS, one_list, 0)
    out_ref[...] = got_ref[...].astype(BF16)


def gather_rows(row, table):
    return pl.pallas_call(
        gather_kernel,
        grid=(LISTS // GATHER_LISTS,),
        in_specs=[
            pl.BlockSpec(memory_space=pltpu.SMEM),
            pl.BlockSpec((ROWS, TOK), lambda g: (0, 0)),
        ],
        out_specs=pl.BlockSpec((GATHER_LISTS * CAP, TOK), lambda g: (g, 0)),
        out_shape=jax.ShapeDtypeStruct((LISTS * CAP, TOK), BF16),
        scratch_shapes=[
            pltpu.VMEM((ROWS, TOK), F32),
            pltpu.VMEM((GATHER_LISTS * CAP, TOK), F32),
        ],
        cost_estimate=pl.CostEstimate(
            flops=20_000_000_000, transcendentals=0, bytes_accessed=6_000_000
        ),
        name="gather_rows",
    )(row, table)


DOT_LISTS = 32


def dots_kernel(cot_ref, value_ref, out_ref):
    place = lax.broadcasted_iota(jnp.int32, (CAP, TOK), 0)
    lane = lax.broadcasted_iota(jnp.int32, (CAP, TOK), 1)
    own = place == lane
    for i in range(DOT_LISTS):
        at = i * CAP
        product = cot_ref[at : at + CAP, :].astype(F32) * value_ref[at : at + CAP, :].astype(F32)
        total = jnp.sum(product, axis=1, keepdims=True)
        out_ref[i : i + 1, :] = jnp.sum(jnp.where(own, total, 0.0), axis=0, keepdims=True)


def dots(cot, value):
    return pl.pallas_call(
        dots_kernel,
        grid=(LISTS // DOT_LISTS,),
        in_specs=[
            pl.BlockSpec((DOT_LISTS * CAP, TOK), lambda g: (g, 0)),
            pl.BlockSpec((DOT_LISTS * CAP, TOK), lambda g: (g, 0)),
        ],
        out_specs=pl.BlockSpec((DOT_LISTS, TOK), lambda g: (g, 0)),
        out_shape=jax.ShapeDtypeStruct((LISTS, TOK), F32),
        name="dots",
    )(cot, value)


SCATTER_LISTS = 8


def scatter_kernel(row_ref, rec_ref, cot_ref, out_ref, sq_ref, wide_ref, *accs):
    step = pl.program_id(0)

    @pl.when(step == 0)
    def _():
        def clear(i, carry):
            at = pl.multiple_of(i * 64, 64)
            for acc in accs:
                acc[pl.ds(at, 64), :] = jnp.zeros((64, TOK), F32)
            return carry

        lax.fori_loop(0, ROWS // 64, clear, 0)

    wide_ref[...] = cot_ref[...].astype(F32)

    def one_list(i, carry):
        which = step * SCATTER_LISTS + i
        count = row_ref[which, 2 * CAP]

        def one_group(g, c):
            for j in range(8):
                slot = g * 8 + j
                row = row_ref[which, slot]
                weight = rec_ref[which, CAP + slot]
                acc = accs[j % ACCS]
                acc[pl.ds(row, 1), :] = (
                    acc[pl.ds(row, 1), :] + wide_ref[pl.ds(i * CAP + slot, 1), :] * weight
                )
            return c

        lax.fori_loop(0, jnp.right_shift(count + 7, 3), one_group, 0)
        return carry

    lax.fori_loop(0, SCATTER_LISTS, one_list, 0)

    @pl.when(step == pl.num_programs(0) - 1)
    def _():
        def collect(i, total):
            at = pl.multiple_of(i * 64, 64)
            value = accs[0][pl.ds(at, 64), :]
            for acc in accs[1:]:
                value = value + acc[pl.ds(at, 64), :]
            out_ref[pl.ds(at, 64), :] = value
            square = value * value
            return total + jnp.sum(square.reshape(8, 8, TOK), axis=0)

        sq_ref[...] = lax.fori_loop(0, ROWS // 64, collect, jnp.zeros((8, TOK), F32))


def scatter_rows(row, record, cot):
    return pl.pallas_call(
        scatter_kernel,
        grid=(LISTS // SCATTER_LISTS,),
        in_specs=[
            pl.BlockSpec(memory_space=pltpu.SMEM),
            pl.BlockSpec(memory_space=pltpu.SMEM),
            pl.BlockSpec((SCATTER_LISTS * CAP, TOK), lambda g: (g, 0)),
        ],
        out_specs=(
            pl.BlockSpec((ROWS, TOK), lambda g: (0, 0)),
            pl.BlockSpec((8, TOK), lambda g: (0, 0)),
        ),
        out_shape=(
            jax.ShapeDtypeStruct((ROWS, TOK), F32),
            jax.ShapeDtypeStruct((8, TOK), F32),
        ),
        scratch_shapes=[pltpu.VMEM((SCATTER_LISTS * CAP, TOK), F32)]
        + [pltpu.VMEM((ROWS, TOK), F32) for _ in range(ACCS)],
        cost_estimate=pl.CostEstimate(
            flops=20_000_000_000, transcendentals=0, bytes_accessed=8_000_000
        ),
        name="scatter_rows",
    )(row, record, cot)


def dscore_kernel(ret_ref, aux_ref, out_ref):
    owner_id = lax.broadcasted_iota(jnp.int32, (TOK, TOK), 0)
    place_id = lax.broadcasted_iota(jnp.int32, (CAP, TOK), 0)
    for s in range(NDP):
        square = jnp.concatenate([ret_ref[:, s, :]] * 4, axis=0)
        columns = jnp.transpose(square)[0:CAP, :]
        parts = pieces(columns)
        target = aux_ref[s, 8:16, :].astype(jnp.int32)
        picked = []
        for k in range(PICKS):
            owner = jnp.right_shift(target[k : k + 1, :], 7)
            place = jnp.bitwise_and(target[k : k + 1, :], TOK - 1)
            chosen = jnp.where(owner_id == owner, 1.0, 0.0).astype(BF16)
            got = lax.dot_general(parts[0], chosen, NN, preferred_element_type=F32)
            got = got + lax.dot_general(parts[1], chosen, NN, preferred_element_type=F32)
            got = got + lax.dot_general(parts[2], chosen, NN, preferred_element_type=F32)
            picked.append(
                jnp.sum(jnp.where(place_id == place, got, 0.0), axis=0, keepdims=True)
            )
        picked = jnp.concatenate(picked, axis=0)
        weight = aux_ref[s, 0:8, :]
        both = weight * picked
        mean0 = jnp.sum(both[0:4, :], axis=0, keepdims=True)
        mean1 = jnp.sum(both[4:8, :], axis=0, keepdims=True)
        row = lax.broadcasted_iota(jnp.int32, (PICKS, TOK), 0)
        out_ref[s * 8 : s * 8 + 8, :] = weight * (picked - jnp.where(row < 4, mean0, mean1))


def partial_dscore(returned, aux):
    return pl.pallas_call(
        dscore_kernel,
        out_shape=jax.ShapeDtypeStruct((NDP * PICKS, TOK), F32),
        name="dscore",
    )(returned, aux)


def key_kernel(ds_ref, aux_ref, q_ref, base_ref, out_ref):
    dscore = ds_ref[0]
    for d in range(1, NDP):
        dscore = dscore + ds_ref[d]
    base = base_ref[0]
    key_id = lax.broadcasted_iota(jnp.int32, (KEYS, TOK), 0) + base
    for half in range(2):
        for head in range(2):
            at = head * 2 * HALF + half * HALF
            blocks = []
            for s in range(NDP):
                index = aux_ref[s, 16 + half * 8 : 24 + half * 8, :].astype(jnp.int32)
                block = jnp.zeros((KEYS, TOK), F32)
                for k in range(4):
                    slot = head * 4 + k
                    value = dscore[s * 8 + slot : s * 8 + slot + 1, :]
                    block = block + jnp.where(key_id == index[slot : slot + 1, :], value, 0.0)
                blocks.append(block)
            weighted = jnp.concatenate(blocks, axis=1)
            total = None
            for piece in pieces(weighted):
                term = lax.dot_general(
                    piece, q_ref[:, at : at + HALF], NN, preferred_element_type=F32
                )
                total = term if total is None else total + term
            out_ref[half, head] = total


def key_terms(dscore, aux, queries, base):
    return pl.pallas_call(
        key_kernel,
        in_specs=[
            pl.BlockSpec(memory_space=pltpu.VMEM),
            pl.BlockSpec(memory_space=pltpu.VMEM),
            pl.BlockSpec(memory_space=pltpu.VMEM),
            pl.BlockSpec(memory_space=pltpu.SMEM),
        ],
        out_shape=jax.ShapeDtypeStruct((2, 2, KEYS, HALF), F32),
        name="key_terms",
    )(dscore, aux, queries, base)


def exchange(x, axis):
    return lax.all_to_all(x, axis, 0, 0, tiled=True)


def everyone(x, axis, size):
    return exchange(jnp.broadcast_to(x[None], (size, *x.shape)), axis)


def local(queries, sub_keys, values, slot_first, slot_second, cotangent):
    q = queries.reshape(TOK, 4 * HALF)
    first = slot_first.reshape(TOK, PICKS).T
    second = slot_second.reshape(TOK, PICKS).T
    cot_columns = exchange(
        jnp.moveaxis(cotangent.reshape(TOK, NDP, TOK), 1, 0), "dp"
    )
    record, aux = prep(q, sub_keys, first, second)
    gathered = everyone(jnp.concatenate([record, aux], axis=0), "dp", NDP)
    records = gathered[:, 0:OWN, :]
    aux_all = gathered[:, OWN:, :]
    received = exchange(jnp.moveaxis(records, 1, 0), TABLE)
    rows = exchange(expand(records, cot_columns), TABLE)
    q_late, _ = lax.optimization_barrier((q, gathered))
    q_all = everyone(q_late, "dp", NDP).reshape(NDP * TOK, 4 * HALF)
    record_mine = received.reshape(LISTS, TOK)
    code = record_mine.astype(jnp.int32)
    lane = lax.broadcasted_iota(jnp.int32, (LISTS, TOK), 1)
    row = jnp.where(lane < CAP, jnp.right_shift(code, 7), code)
    value_rows = gather_rows(row, values.reshape(ROWS, TOK))
    rows_flat = rows.reshape(LISTS * CAP, TOK)
    partial = dots(rows_flat, value_rows)
    returned = exchange(partial.reshape(OWN, NDP, TOK), TABLE)
    value_grad, value_sq = scatter_rows(row, record_mine, rows_flat)
    dscore = everyone(partial_dscore(returned, aux_all), "dp", NDP)
    base = (lax.axis_index("dp") * KEYS).astype(jnp.int32).reshape(1)
    key_grad = key_terms(dscore, aux_all, q_all, base)
    key_blocks = jnp.moveaxis(key_grad.reshape(2, 2, OWN, 2, HALF), 2, 0)
    key_part = jnp.sum(exchange(key_blocks.reshape(OWN, 8, HALF), TABLE), axis=0)
    local_sq = jnp.sum(value_sq) + jnp.sum(key_part * key_part)
    total_sq = jnp.sum(everyone(local_sq.reshape(1), ALL, OWN * NDP))
    clip_factor = jnp.minimum(1.0, LIMIT_RATIO * math.sqrt(TOK * OWN * NDP) / jnp.sqrt(total_sq))
    value_update = (clip_factor * value_grad).reshape(BLK, NSUB, TOK)
    key_update = (clip_factor * key_part).reshape(2, 2, 2, HALF)
    return (value_update, key_update, clip_factor.reshape(1))


def solution(mesh):
    torus = Mesh(
        mesh.devices.reshape(mesh.shape["dp"], 4, 4, 2), ("dp", "table_0", "table_1", "table_2")
    )
    return jax.shard_map(
        local,
        mesh=torus,
        in_specs=(
            P(DP_TABLE, None, None),
            P(),
            P(TABLE, None, "dp"),
            P(DP_TABLE, None, None),
            P(DP_TABLE, None, None),
            P(DP_TABLE, None),
        ),
        out_specs=(P(TABLE, None, "dp"), P(None, None, DP_TABLE, None), P()),
        check_vma=False,
    )
```

```python
import functools
import math

import jax
import jax.numpy as jnp
from jax import lax
from jax.experimental import pallas as pl
from jax.experimental.pallas import tpu as pltpu
from jax.sharding import Mesh
from jax.sharding import PartitionSpec as P


TABLE = ("table_0", "table_1", "table_2")
DP_TABLE = ("dp", "table_0", "table_1", "table_2")
CHIPS = ("dp", "table_0", "table_1")
NSUB = 512
BLK = 16
CAP = 48
OWN = 32
NDP = 8
TOK = 128
PICKS = 8
HALF = 256
KEYS = NSUB // NDP
LISTS = OWN * NDP
PART = NDP // 2
PART_LISTS = OWN * PART
ROWS = BLK * NSUB
RECORDS = 2 * NDP
ACCS = 8
BATCH = 4
EXTRA = 16
F32 = jnp.float32
BF16 = jnp.bfloat16
LIMIT_RATIO = 5.0

NT = (((1,), (1,)), ((), ()))
NN = (((1,), (0,)), ((), ()))

PARAMS = pltpu.CompilerParams(vmem_limit_bytes=20 * 1024 * 1024)


def pieces(x):
    high = x.astype(BF16)
    rest = x - high.astype(F32)
    mid = rest.astype(BF16)
    low = (rest - mid.astype(F32)).astype(BF16)
    return high, mid, low


def joined(high, mid, low):
    return (high.astype(F32) + mid.astype(F32)) + low.astype(F32)


def vmem(count):
    return [pl.BlockSpec(memory_space=pltpu.VMEM)] * count


def smem():
    return [pl.BlockSpec(memory_space=pltpu.SMEM)]


def shape(dims, kind):
    return jax.ShapeDtypeStruct(dims, kind)


def prep_kernel(q_ref, keys_ref, first_ref, second_ref, cot_ref, out_ref, late_ref):
    first = first_ref[...]
    second = second_ref[...]
    key_id = lax.broadcasted_iota(jnp.int32, (NSUB, TOK), 0)
    scores = [None] * PICKS
    for half, index in ((0, first), (1, second)):
        for head in range(2):
            at = head * 2 * HALF + half * HALF
            table = lax.dot_general(
                keys_ref[half, head], q_ref[:, at : at + HALF], NT, preferred_element_type=F32
            )
            for k in range(4):
                slot = head * 4 + k
                part = jnp.sum(
                    jnp.where(key_id == index[slot : slot + 1, :], table, 0.0),
                    axis=0,
                    keepdims=True,
                )
                scores[slot] = part if scores[slot] is None else scores[slot] + part
    exps = [jnp.exp(s) for s in scores]
    weights = []
    for head in range(2):
        e = exps[head * 4 : head * 4 + 4]
        total = (e[0] + e[1]) + (e[2] + e[3])
        weights += [x / total for x in e]
    owner = jnp.right_shift(first, 4)
    owner_id = lax.broadcasted_iota(jnp.int32, (OWN, TOK), 0)
    member = [
        jnp.where(owner_id == owner[s : s + 1, :], 1.0, 0.0).astype(F32) for s in range(PICKS)
    ]
    earlier = jnp.where(
        lax.broadcasted_iota(jnp.int32, (TOK, TOK), 0)
        < lax.broadcasted_iota(jnp.int32, (TOK, TOK), 1),
        1.0,
        0.0,
    ).astype(BF16)
    member_all = jnp.concatenate(member, axis=0).astype(BF16)
    ranks = lax.dot_general(member_all, earlier, NN, preferred_element_type=F32)
    base = jnp.zeros((OWN, 1), F32)
    token = lax.broadcasted_iota(jnp.int32, (1, TOK), 1).astype(F32)
    lane_id = lax.broadcasted_iota(jnp.int32, (TOK, TOK), 0)
    planes = [jnp.zeros((OWN, TOK), F32)] * 2
    targets = []
    for s in range(PICKS):
        rank = jnp.sum(
            member[s] * (ranks[s * OWN : (s + 1) * OWN, :] + base), axis=0, keepdims=True
        )
        base = base + jnp.sum(member[s], axis=1, keepdims=True)
        place = rank.astype(jnp.int32)
        row = jnp.bitwise_and(first[s : s + 1, :], BLK - 1) * NSUB + second[s : s + 1, :]
        at_value = lane_id == place
        at_rest = lane_id == place + CAP
        at_token = (
            lane_id == place + 2 * CAP,
            lane_id == jnp.where(place >= TOK - 2 * CAP, place + 4 * CAP - TOK, -1),
        )
        weight = pieces(weights[s])
        parts = (
            (jnp.right_shift(row, 5).astype(F32), jnp.bitwise_and(row, 31).astype(F32)),
            (weight[0].astype(F32), weight[1].astype(F32)),
        )
        chosen = member[s].astype(BF16)
        for p in range(2):
            entry = jnp.where(
                at_value,
                parts[p][0],
                jnp.where(at_rest, parts[p][1], jnp.where(at_token[p], token, 0.0)),
            ).astype(BF16)
            planes[p] = planes[p] + lax.dot_general(
                chosen, entry, NT, preferred_element_type=F32
            )
        targets.append(owner[s : s + 1, :] * TOK + place)
    planes = [plane.astype(BF16) for plane in planes]
    for d in range(NDP):
        out_ref[d, 0:TOK, :] = cot_ref[:, d * TOK : (d + 1) * TOK]
        for p in range(2):
            out_ref[d, TOK + p * OWN : TOK + (p + 1) * OWN, :] = planes[p]
    late_ref[0:TOK, :] = q_ref[...]
    parts = list(pieces(jnp.concatenate(weights, axis=0)))
    for index in (jnp.concatenate(targets, axis=0), first, second):
        parts += [
            jnp.right_shift(index, 6).astype(F32).astype(BF16),
            jnp.bitwise_and(index, 63).astype(F32).astype(BF16),
        ]
    parts = [part.astype(F32) for part in parts]
    parts += [jnp.zeros((PICKS, TOK), F32)] * (EXTRA - len(parts))
    for s in range(PICKS):
        late_ref[TOK : TOK + EXTRA, s * TOK : (s + 1) * TOK] = jnp.concatenate(
            [part[s : s + 1, :] for part in parts], axis=0
        ).astype(BF16)


def prep(q, keys, first, second, cot):
    return pl.pallas_call(
        prep_kernel,
        in_specs=vmem(5),
        out_specs=vmem(2),
        out_shape=(
            shape((NDP, TOK + 2 * OWN, TOK), BF16),
            shape((TOK + EXTRA, 4 * HALF), BF16),
        ),
        compiler_params=PARAMS,
        name="prep",
    )(q, keys, first, second, cot)


def late_index(late_ref, slot, part):
    at = slice(slot * TOK, (slot + 1) * TOK)
    high = late_ref[part : part + 1, at].astype(F32).astype(jnp.int32)
    low = late_ref[part + 1 : part + 2, at].astype(F32).astype(jnp.int32)
    return high * 64 + low


def source(me, k):
    return jnp.bitwise_and(me + NDP - k, NDP - 1)


def expand_kernel(part, sent_ref, out_ref, *scratch):
    lane = lax.broadcasted_iota(jnp.int32, (CAP, TOK), 1)
    for k in range(PART):
        s = part * PART + k
        planes = [sent_ref[s, TOK + p * OWN : TOK + (p + 1) * OWN, :].astype(F32) for p in range(2)]
        columns = [jnp.transpose(jnp.concatenate([plane] * 4, axis=0)) for plane in planes]
        token = jnp.concatenate(
            [columns[0][2 * CAP : TOK, :], columns[1][2 * CAP : 5 * CAP - TOK, :]], axis=0
        ).astype(jnp.int32)
        chosen = jnp.concatenate(
            [
                jnp.where(token[:, o : o + 1] == lane, 1.0, 0.0).astype(BF16)
                for o in range(OWN)
            ],
            axis=0,
        )
        out_ref[:, k * CAP : (k + 1) * CAP, :] = (
            lax.dot_general(chosen, sent_ref[s, 0:TOK, :], NN, preferred_element_type=F32)
            .astype(BF16)
            .reshape(OWN, CAP, TOK)
        )
    if part == 0:
        wide_ref = scratch[0]
        for s in range(NDP):
            for p in range(2):
                wide_ref[:, 2 * s + p, :] = sent_ref[
                    s, TOK + p * OWN : TOK + (p + 1) * OWN, :
                ].astype(F32)
        out_ref[:, PART * CAP :, :] = wide_ref[...].astype(BF16)


def expand(part, sent):
    extra = RECORDS if part == 0 else 0
    return pl.pallas_call(
        functools.partial(expand_kernel, part),
        in_specs=vmem(1),
        out_specs=vmem(1)[0],
        out_shape=shape((OWN, PART * CAP + extra, TOK), BF16),
        scratch_shapes=[pltpu.VMEM((OWN, RECORDS, TOK), F32)] if part == 0 else [],
        compiler_params=PARAMS,
        name="expand",
    )(sent)


def decode_kernel(rows_ref, row_ref, weight_ref, wide_ref):
    for t in range(OWN):
        wide_ref[t * RECORDS : (t + 1) * RECORDS, :] = rows_ref[t, PART * CAP :, :].astype(F32)
    index = wide_ref[pl.ds(0, LISTS, stride=2), :]
    weight = wide_ref[pl.ds(1, LISTS, stride=2), :]
    row_ref[...] = (index * 32.0 + pltpu.roll(index, TOK - CAP, 1)).astype(jnp.int32)
    weight_ref[...] = weight + pltpu.roll(weight, TOK - CAP, 1)


def decode(rows):
    return pl.pallas_call(
        decode_kernel,
        in_specs=vmem(1),
        out_specs=vmem(2),
        out_shape=(shape((LISTS, TOK), jnp.int32), shape((LISTS, TOK), F32)),
        scratch_shapes=[pltpu.VMEM((OWN * RECORDS, TOK), F32)],
        compiler_params=PARAMS,
        name="decode",
    )(rows)


GATHER_LISTS = 32


def gather_kernel(row_ref, table_ref, out_ref, wide_ref, got_ref):
    step = pl.program_id(0)

    @pl.when(step == 0)
    def _():
        def widen(i, carry):
            at = pl.multiple_of(i * 256, 256)
            wide_ref[pl.ds(at, 256), :] = table_ref[pl.ds(at, 256), :].astype(F32)
            return carry

        lax.fori_loop(0, ROWS // 256, widen, 0)

    part = step // (PART_LISTS // GATHER_LISTS)
    first_list = (step % (PART_LISTS // GATHER_LISTS)) * GATHER_LISTS

    def one_list(i, carry):
        at = first_list + i
        which = (at // PART) * NDP + part * PART + at % PART
        for j in range(CAP):
            row = row_ref[which, j]
            got_ref[pl.ds(i * CAP + j, 1), :] = wide_ref[pl.ds(row, 1), :]
        return carry

    lax.fori_loop(0, GATHER_LISTS, one_list, 0)
    out_ref[...] = got_ref[...].astype(BF16)


def gather_rows(row, table):
    return pl.pallas_call(
        gather_kernel,
        grid=(LISTS // GATHER_LISTS,),
        in_specs=smem() + [pl.BlockSpec((ROWS, TOK), lambda g: (0, 0))],
        out_specs=pl.BlockSpec((GATHER_LISTS * CAP, TOK), lambda g: (g, 0)),
        out_shape=shape((LISTS * CAP, TOK), BF16),
        scratch_shapes=[
            pltpu.VMEM((ROWS, TOK), F32),
            pltpu.VMEM((GATHER_LISTS * CAP, TOK), F32),
        ],
        compiler_params=PARAMS,
        name="gather_rows",
    )(row, table)


DOT_OWN = 8


def dots_kernel(part, *refs):
    rows_ref, value_ref = refs[:2]
    out_ref = refs[-1]
    place = lax.broadcasted_iota(jnp.int32, (CAP, TOK), 0)
    lane = lax.broadcasted_iota(jnp.int32, (CAP, TOK), 1)
    own = place == lane
    made = []
    for t in range(DOT_OWN):
        if part == 1:
            made.append(refs[2][t * PART : (t + 1) * PART, :])
        for k in range(PART):
            at = (t * PART + k) * CAP
            product = rows_ref[t, k * CAP : (k + 1) * CAP, :].astype(F32) * value_ref[
                at : at + CAP, :
            ].astype(F32)
            total = jnp.sum(product, axis=1, keepdims=True)
            made.append(jnp.sum(jnp.where(own, total, 0.0), axis=0, keepdims=True))
    out_ref[...] = jnp.concatenate(made, axis=0)


def dots(part, rows, value, earlier=()):
    steps = OWN // DOT_OWN
    count = DOT_OWN * (PART if part == 0 else NDP)
    return pl.pallas_call(
        functools.partial(dots_kernel, part),
        grid=(steps,),
        in_specs=[
            pl.BlockSpec((DOT_OWN, rows.shape[1], TOK), lambda g: (g, 0, 0)),
            pl.BlockSpec((DOT_OWN * PART * CAP, TOK), lambda g: (part * steps + g, 0)),
        ]
        + [pl.BlockSpec((DOT_OWN * PART, TOK), lambda g: (g, 0))] * len(earlier),
        out_specs=pl.BlockSpec((count, TOK), lambda g: (g, 0)),
        out_shape=shape((count * steps, TOK), F32),
        compiler_params=PARAMS,
        name="dots",
    )(rows, value, *earlier)


SCATTER_OWN = 8
SCATTER_STEPS = OWN // SCATTER_OWN


def scatter_kernel(row_ref, weight_ref, rows_a_ref, rows_b_ref, out_ref, sq_ref, wide_ref, *accs):
    step = pl.program_id(0)

    @pl.when(step == 0)
    def _():
        def clear(i, carry):
            at = pl.multiple_of(i * 64, 64)
            for acc in accs:
                acc[pl.ds(at, 64), :] = jnp.zeros((64, TOK), F32)
            return carry

        lax.fori_loop(0, ROWS // 64, clear, 0)

    block = step % SCATTER_STEPS
    part = step // SCATTER_STEPS
    at = pl.multiple_of(block * SCATTER_OWN * NDP, SCATTER_OWN * NDP)
    weight = weight_ref[pl.ds(at, SCATTER_OWN * NDP), :]
    columns = jnp.transpose(jnp.concatenate([weight] * (TOK // (SCATTER_OWN * NDP)), axis=0))
    for which, rows_ref in ((0, rows_a_ref), (1, rows_b_ref)):

        @pl.when(part == which)
        def _():
            for t in range(SCATTER_OWN):
                for k in range(PART):
                    i = t * PART + k
                    s = t * NDP + which * PART + k
                    wide_ref[i * CAP : (i + 1) * CAP, :] = (
                        rows_ref[t, k * CAP : (k + 1) * CAP, :].astype(F32)
                        * columns[0:CAP, s : s + 1]
                    )

    def one_list(i, carry):
        which = (block * SCATTER_OWN + i // PART) * NDP + part * PART + i % PART
        waiting = []
        for b in range(0, CAP, BATCH):
            made = []
            for j in range(b, b + BATCH):
                acc = accs[j % ACCS]
                row = row_ref[which, j]
                made.append((acc, row, acc[pl.ds(row, 1), :] + wide_ref[pl.ds(i * CAP + j, 1), :]))
            for acc, row, total in waiting:
                acc[pl.ds(row, 1), :] = total
            waiting = made
        for acc, row, total in waiting:
            acc[pl.ds(row, 1), :] = total
        return carry

    lax.fori_loop(0, SCATTER_OWN * PART, one_list, 0)

    @pl.when(step == pl.num_programs(0) - 1)
    def _():
        def collect(i, total):
            at = pl.multiple_of(i * 64, 64)
            value = accs[0][pl.ds(at, 64), :]
            for acc in accs[1:]:
                value = value + acc[pl.ds(at, 64), :]
            out_ref[pl.ds(at, 64), :] = value
            square = value * value
            return total + jnp.sum(square.reshape(8, 8, TOK), axis=0)

        sq_ref[...] = lax.fori_loop(0, ROWS // 64, collect, jnp.zeros((8, TOK), F32))


def scatter_rows(row, weight, rows_a, rows_b):
    last = SCATTER_STEPS - 1
    return pl.pallas_call(
        scatter_kernel,
        grid=(2 * SCATTER_STEPS,),
        in_specs=smem()
        + vmem(1)
        + [
            pl.BlockSpec(
                (SCATTER_OWN, rows_a.shape[1], TOK), lambda g: (jnp.minimum(g, last), 0, 0)
            ),
            pl.BlockSpec(
                (SCATTER_OWN, rows_b.shape[1], TOK),
                lambda g: (jnp.maximum(g - SCATTER_STEPS, 0), 0, 0),
            ),
        ],
        out_specs=vmem(2),
        out_shape=(shape((ROWS, TOK), F32), shape((8, TOK), F32)),
        scratch_shapes=[pltpu.VMEM((SCATTER_OWN * PART * CAP, TOK), F32)]
        + [pltpu.VMEM((ROWS, TOK), F32) for _ in range(ACCS)],
        compiler_params=pltpu.CompilerParams(vmem_limit_bytes=52 * 1024 * 1024),
        name="scatter_rows",
    )(row, weight, rows_a, rows_b)


SCALE_ROWS = 1024


def scale_kernel(factor_ref, value_ref, out_ref):
    out_ref[...] = value_ref[...] * factor_ref[0]


def scaled(factor, value):
    return pl.pallas_call(
        scale_kernel,
        grid=(ROWS // SCALE_ROWS,),
        in_specs=smem() + [pl.BlockSpec((SCALE_ROWS, TOK), lambda g: (g, 0))],
        out_specs=pl.BlockSpec((SCALE_ROWS, TOK), lambda g: (g, 0)),
        out_shape=shape((ROWS, TOK), F32),
        compiler_params=PARAMS,
        name="scale",
    )(factor, value)


def dscore_kernel(me_ref, ret_ref, *refs):
    late_refs = refs[:NDP]
    out_ref = refs[NDP]
    owner_id = lax.broadcasted_iota(jnp.int32, (OWN, TOK), 0)
    place_id = lax.broadcasted_iota(jnp.int32, (CAP, TOK), 0)
    row = lax.broadcasted_iota(jnp.int32, (PICKS, TOK), 0)
    for s in range(NDP):
        late_ref = late_refs[s]
        which = source(me_ref[0], s)
        square = jnp.concatenate([ret_ref[:, which, :]] * 4, axis=0)
        columns = jnp.transpose(square)[0:CAP, 0:OWN]
        stacked = jnp.concatenate(pieces(columns), axis=0)
        target = [late_index(late_ref, k, 3) for k in range(PICKS)]
        chosen = jnp.concatenate(
            [
                jnp.where(owner_id == jnp.right_shift(target[k], 7), 1.0, 0.0).astype(BF16)
                for k in range(PICKS)
            ],
            axis=1,
        )
        got = lax.dot_general(stacked, chosen, NN, preferred_element_type=F32)
        got = (got[0:CAP, :] + got[CAP : 2 * CAP, :]) + got[2 * CAP : 3 * CAP, :]
        picked = jnp.concatenate(
            [
                jnp.sum(
                    jnp.where(
                        place_id == jnp.bitwise_and(target[k], TOK - 1),
                        got[:, k * TOK : (k + 1) * TOK],
                        0.0,
                    ),
                    axis=0,
                    keepdims=True,
                )
                for k in range(PICKS)
            ],
            axis=0,
        )
        weight = jnp.concatenate(
            [
                joined(*[late_ref[p : p + 1, k * TOK : (k + 1) * TOK] for p in range(3)])
                for k in range(PICKS)
            ],
            axis=0,
        )
        both = weight * picked
        mean0 = jnp.sum(both[0:4, :], axis=0, keepdims=True)
        mean1 = jnp.sum(both[4:8, :], axis=0, keepdims=True)
        at = pl.multiple_of(which * 8, 8)
        slope = weight * (picked - jnp.where(row < 4, mean0, mean1))
        for d in range(NDP):
            out_ref[d, pl.ds(at, 8), :] = slope


def partial_dscore(me, returned, late):
    return pl.pallas_call(
        dscore_kernel,
        grid=(1,),
        in_specs=smem()
        + vmem(1)
        + [pl.BlockSpec((EXTRA, 4 * HALF), lambda g: (TOK // EXTRA, 0))] * NDP,
        out_specs=vmem(1)[0],
        out_shape=shape((NDP, NDP * PICKS, TOK), F32),
        compiler_params=PARAMS,
        name="dscore",
    )(me, returned, *late)


def key_kernel(me_ref, ds_ref, *refs):
    late_refs = refs[:NDP]
    out_ref = refs[NDP]
    base = me_ref[0] * KEYS
    dscore = []
    for s in range(NDP):
        at = pl.multiple_of(source(me_ref[0], s) * 8, 8)
        total = ds_ref[0, pl.ds(at, 8), :]
        for d in range(1, NDP):
            total = total + ds_ref[d, pl.ds(at, 8), :]
        dscore.append(total)
    key_id = lax.broadcasted_iota(jnp.int32, (KEYS, TOK), 0) + base
    for half in range(2):
        for head in range(2):
            at = head * 2 * HALF + half * HALF
            blocks = []
            for s in range(NDP):
                block = jnp.zeros((KEYS, TOK), F32)
                for k in range(4):
                    slot = head * 4 + k
                    value = dscore[s][slot : slot + 1, :]
                    block = block + jnp.where(
                        key_id == late_index(late_refs[s], slot, TOK + 5 + 2 * half), value, 0.0
                    )
                blocks.append(block)
            weighted = jnp.concatenate(blocks, axis=1)
            query = jnp.concatenate(
                [late_refs[s][0:TOK, at : at + HALF] for s in range(NDP)], axis=0
            )
            stacked = jnp.concatenate(pieces(weighted), axis=0)
            total = lax.dot_general(stacked, query, NN, preferred_element_type=F32)
            total = (total[0:KEYS, :] + total[KEYS : 2 * KEYS, :]) + total[2 * KEYS : 3 * KEYS, :]
            r = half * 4 + head * 2
            out_ref[:, r : r + 2, :] = total.reshape(OWN, 2, HALF)


def key_terms(me, dscore, late):
    return pl.pallas_call(
        key_kernel,
        in_specs=smem() + vmem(1 + NDP),
        out_specs=vmem(1)[0],
        out_shape=shape((OWN, 8, HALF), F32),
        compiler_params=PARAMS,
        name="key_terms",
    )(me, dscore, *late)


def exchange(x, axis):
    return lax.all_to_all(x, axis, 0, 0, tiled=True)


def everyone(x, axis, size):
    return exchange(jnp.broadcast_to(x[None], (size, *x.shape)), axis)


def body(queries, sub_keys, values, slot_first, slot_second, cotangent):
    q = queries.reshape(TOK, 4 * HALF)
    first = slot_first.reshape(TOK, PICKS).T
    second = slot_second.reshape(TOK, PICKS).T
    me = lax.axis_index("dp").astype(jnp.int32).reshape(1)
    outgoing, late = prep(q, sub_keys, first, second, cotangent)
    sent = exchange(outgoing, "dp")
    expanded = expand(0, sent)
    rows_a = exchange(expanded, TABLE)
    expanded = expand(1, sent)
    rows_b = exchange(expanded, TABLE)
    late, _ = lax.optimization_barrier((late, sent))
    late_all = [late] + [
        lax.ppermute(late, "dp", [(i, (i + k) % NDP) for i in range(NDP)])
        for k in range(1, NDP)
    ]
    row, weight = decode(rows_a)
    value_rows = gather_rows(row, values.reshape(ROWS, TOK))
    partial = dots(0, rows_a, value_rows)
    partial = dots(1, rows_b, value_rows, (partial,))
    returned = exchange(partial.reshape(OWN, NDP, TOK), TABLE)
    value_grad, value_sq = scatter_rows(row, weight, rows_a, rows_b)
    slopes = partial_dscore(me, returned, late_all)
    dscore = exchange(slopes, "dp")
    key_grad = key_terms(me, dscore, late_all)
    key_pieces = exchange(key_grad, TABLE)
    key_part = jnp.sum(key_pieces, axis=0)
    local_sq = (jnp.sum(value_sq) + jnp.sum(key_part * key_part)).reshape(1)
    chip_sq = local_sq + lax.ppermute(local_sq, "table_2", [(0, 1), (1, 0)])
    total_sq = jnp.sum(everyone(chip_sq, CHIPS, OWN * NDP // 2))
    clip_factor = jnp.minimum(
        1.0, LIMIT_RATIO * math.sqrt(TOK * OWN * NDP) / jnp.sqrt(total_sq)
    ).reshape(1)
    value_update = scaled(clip_factor, value_grad).reshape(BLK, NSUB, TOK)
    key_update = (clip_factor[0] * key_part).reshape(2, 2, 2, HALF)
    return (value_update, key_update, clip_factor)


def solution(mesh):
    torus = Mesh(
        mesh.devices.reshape(mesh.shape["dp"], 4, 4, 2), ("dp", "table_0", "table_1", "table_2")
    )
    return jax.shard_map(
        body,
        mesh=torus,
        in_specs=(
            P(DP_TABLE, None, None),
            P(),
            P(TABLE, None, "dp"),
            P(DP_TABLE, None, None),
            P(DP_TABLE, None, None),
            P(DP_TABLE, None),
        ),
        out_specs=(P(TABLE, None, "dp"), P(None, None, DP_TABLE, None), P()),
        check_vma=False,
    )
```

```python
import functools
import math

import jax
import jax.numpy as jnp
from jax import lax
from jax.experimental import pallas as pl
from jax.experimental.pallas import tpu as pltpu
from jax.sharding import Mesh
from jax.sharding import PartitionSpec as P


TABLE = ("table_0", "table_1", "table_2")
DP_TABLE = ("dp", "table_0", "table_1", "table_2")
CHIPS = ("dp", "table_0", "table_1")
NSUB = 512
BLK = 16
CAP = 48
OWN = 32
NDP = 8
TOK = 128
PICKS = 8
HALF = 256
KEYS = NSUB // NDP
LISTS = OWN * NDP
PART = NDP // 2
ROWS = BLK * NSUB
RECORDS = 2 * NDP
ACCS = 8
BATCH = 4
EXTRA = 16
F32 = jnp.float32
BF16 = jnp.bfloat16
LIMIT_RATIO = 5.0

NT = (((1,), (1,)), ((), ()))
NN = (((1,), (0,)), ((), ()))

PARAMS = pltpu.CompilerParams(vmem_limit_bytes=20 * 1024 * 1024)


def pieces(x):
    high = x.astype(BF16)
    rest = x - high.astype(F32)
    mid = rest.astype(BF16)
    low = (rest - mid.astype(F32)).astype(BF16)
    return high, mid, low


def joined(high, mid, low):
    return (high.astype(F32) + mid.astype(F32)) + low.astype(F32)


def vmem(count):
    return [pl.BlockSpec(memory_space=pltpu.VMEM)] * count


def smem():
    return [pl.BlockSpec(memory_space=pltpu.SMEM)]


def shape(dims, kind):
    return jax.ShapeDtypeStruct(dims, kind)


def prep_kernel(q_ref, keys_ref, first_ref, second_ref, cot_ref, out_ref, late_ref):
    first = first_ref[...]
    second = second_ref[...]
    key_id = lax.broadcasted_iota(jnp.int32, (NSUB, TOK), 0)
    scores = [None] * PICKS
    for half, index in ((0, first), (1, second)):
        for head in range(2):
            at = head * 2 * HALF + half * HALF
            table = lax.dot_general(
                keys_ref[half, head], q_ref[:, at : at + HALF], NT, preferred_element_type=F32
            )
            for k in range(4):
                slot = head * 4 + k
                part = jnp.sum(
                    jnp.where(key_id == index[slot : slot + 1, :], table, 0.0),
                    axis=0,
                    keepdims=True,
                )
                scores[slot] = part if scores[slot] is None else scores[slot] + part
    exps = [jnp.exp(s) for s in scores]
    weights = []
    for head in range(2):
        e = exps[head * 4 : head * 4 + 4]
        total = (e[0] + e[1]) + (e[2] + e[3])
        weights += [x / total for x in e]
    owner = jnp.right_shift(first, 4)
    owner_id = lax.broadcasted_iota(jnp.int32, (OWN, TOK), 0)
    member = [
        jnp.where(owner_id == owner[s : s + 1, :], 1.0, 0.0).astype(F32) for s in range(PICKS)
    ]
    earlier = jnp.where(
        lax.broadcasted_iota(jnp.int32, (TOK, TOK), 0)
        < lax.broadcasted_iota(jnp.int32, (TOK, TOK), 1),
        1.0,
        0.0,
    ).astype(BF16)
    member_all = jnp.concatenate(member, axis=0).astype(BF16)
    ranks = lax.dot_general(member_all, earlier, NN, preferred_element_type=F32)
    base = jnp.zeros((OWN, 1), F32)
    token = lax.broadcasted_iota(jnp.int32, (1, TOK), 1).astype(F32)
    lane_id = lax.broadcasted_iota(jnp.int32, (TOK, TOK), 0)
    planes = [jnp.zeros((OWN, TOK), F32)] * 2
    targets = []
    for s in range(PICKS):
        rank = jnp.sum(
            member[s] * (ranks[s * OWN : (s + 1) * OWN, :] + base), axis=0, keepdims=True
        )
        base = base + jnp.sum(member[s], axis=1, keepdims=True)
        place = rank.astype(jnp.int32)
        row = jnp.bitwise_and(first[s : s + 1, :], BLK - 1) * NSUB + second[s : s + 1, :]
        at_value = lane_id == place
        at_rest = lane_id == place + CAP
        at_token = (
            lane_id == place + 2 * CAP,
            lane_id == jnp.where(place >= TOK - 2 * CAP, place + 4 * CAP - TOK, -1),
        )
        weight = pieces(weights[s])
        parts = (
            (jnp.right_shift(row, 5).astype(F32), jnp.bitwise_and(row, 31).astype(F32)),
            (weight[0].astype(F32), weight[1].astype(F32)),
        )
        chosen = member[s].astype(BF16)
        for p in range(2):
            entry = jnp.where(
                at_value,
                parts[p][0],
                jnp.where(at_rest, parts[p][1], jnp.where(at_token[p], token, 0.0)),
            ).astype(BF16)
            planes[p] = planes[p] + lax.dot_general(
                chosen, entry, NT, preferred_element_type=F32
            )
        targets.append(owner[s : s + 1, :] * TOK + place)
    planes = [plane.astype(BF16) for plane in planes]
    for d in range(NDP):
        out_ref[d, 0:TOK, :] = cot_ref[:, d * TOK : (d + 1) * TOK]
        for p in range(2):
            out_ref[d, TOK + p * OWN : TOK + (p + 1) * OWN, :] = planes[p]
    late_ref[0:TOK, :] = q_ref[...]
    parts = list(pieces(jnp.concatenate(weights, axis=0)))
    for index in (jnp.concatenate(targets, axis=0), first, second):
        parts += [
            jnp.right_shift(index, 6).astype(F32).astype(BF16),
            jnp.bitwise_and(index, 63).astype(F32).astype(BF16),
        ]
    parts = [part.astype(F32) for part in parts]
    parts += [jnp.zeros((PICKS, TOK), F32)] * (EXTRA - len(parts))
    for s in range(PICKS):
        late_ref[TOK : TOK + EXTRA, s * TOK : (s + 1) * TOK] = jnp.concatenate(
            [part[s : s + 1, :] for part in parts], axis=0
        ).astype(BF16)


def prep(q, keys, first, second, cot):
    return pl.pallas_call(
        prep_kernel,
        in_specs=vmem(5),
        out_specs=vmem(2),
        out_shape=(
            shape((NDP, TOK + 2 * OWN, TOK), BF16),
            shape((TOK + EXTRA, 4 * HALF), BF16),
        ),
        compiler_params=PARAMS,
        name="prep",
    )(q, keys, first, second, cot)


def late_index(late_ref, slot, part):
    at = slice(slot * TOK, (slot + 1) * TOK)
    high = late_ref[part : part + 1, at].astype(F32).astype(jnp.int32)
    low = late_ref[part + 1 : part + 2, at].astype(F32).astype(jnp.int32)
    return high * 64 + low


def source(me, k):
    return jnp.bitwise_and(me + NDP - k, NDP - 1)


def expand_kernel(part, sent_ref, out_ref, *scratch):
    lane = lax.broadcasted_iota(jnp.int32, (CAP, TOK), 1)
    for k in range(PART):
        s = part * PART + k
        planes = [sent_ref[s, TOK + p * OWN : TOK + (p + 1) * OWN, :].astype(F32) for p in range(2)]
        columns = [jnp.transpose(jnp.concatenate([plane] * 4, axis=0)) for plane in planes]
        token = jnp.concatenate(
            [columns[0][2 * CAP : TOK, :], columns[1][2 * CAP : 5 * CAP - TOK, :]], axis=0
        ).astype(jnp.int32)
        chosen = jnp.concatenate(
            [
                jnp.where(token[:, o : o + 1] == lane, 1.0, 0.0).astype(BF16)
                for o in range(OWN)
            ],
            axis=0,
        )
        out_ref[:, k * CAP : (k + 1) * CAP, :] = (
            lax.dot_general(chosen, sent_ref[s, 0:TOK, :], NN, preferred_element_type=F32)
            .astype(BF16)
            .reshape(OWN, CAP, TOK)
        )
    if part == 0:
        wide_ref = scratch[0]
        for s in range(NDP):
            for p in range(2):
                wide_ref[:, 2 * s + p, :] = sent_ref[
                    s, TOK + p * OWN : TOK + (p + 1) * OWN, :
                ].astype(F32)
        out_ref[:, PART * CAP :, :] = wide_ref[...].astype(BF16)


def expand(part, sent):
    extra = RECORDS if part == 0 else 0
    return pl.pallas_call(
        functools.partial(expand_kernel, part),
        in_specs=vmem(1),
        out_specs=vmem(1)[0],
        out_shape=shape((OWN, PART * CAP + extra, TOK), BF16),
        scratch_shapes=[pltpu.VMEM((OWN, RECORDS, TOK), F32)] if part == 0 else [],
        compiler_params=PARAMS,
        name="expand",
    )(sent)


def decode_kernel(rows_ref, row_ref, weight_ref, wide_ref):
    for t in range(OWN):
        wide_ref[t * RECORDS : (t + 1) * RECORDS, :] = rows_ref[t, PART * CAP :, :].astype(F32)
    for s in range(NDP):
        index = wide_ref[pl.ds(2 * s, OWN, stride=RECORDS), :]
        weight = wide_ref[pl.ds(2 * s + 1, OWN, stride=RECORDS), :]
        at = slice(s * OWN, (s + 1) * OWN)
        row_ref[at, :] = (index * 32.0 + pltpu.roll(index, TOK - CAP, 1)).astype(jnp.int32)
        weight_ref[at, :] = weight + pltpu.roll(weight, TOK - CAP, 1)


def decode(rows):
    return pl.pallas_call(
        decode_kernel,
        in_specs=vmem(1),
        out_specs=vmem(2),
        out_shape=(shape((LISTS, TOK), jnp.int32), shape((LISTS, TOK), F32)),
        scratch_shapes=[pltpu.VMEM((OWN * RECORDS, TOK), F32)],
        compiler_params=PARAMS,
        name="decode",
    )(rows)


def gather_kernel(row_ref, table_ref, out_ref, wide_ref, got_ref):
    @pl.when(pl.program_id(0) == 0)
    def _():
        def widen(i, carry):
            at = pl.multiple_of(i * 256, 256)
            wide_ref[pl.ds(at, 256), :] = table_ref[pl.ds(at, 256), :].astype(F32)
            return carry

        lax.fori_loop(0, ROWS // 256, widen, 0)

    for t in range(OWN):
        for j in range(CAP):
            row = row_ref[t, j]
            got_ref[pl.ds(t * CAP + j, 1), :] = wide_ref[pl.ds(row, 1), :]
    out_ref[...] = got_ref[...].astype(BF16).reshape(1, OWN, CAP, TOK)


def gather_rows(row, table):
    return pl.pallas_call(
        gather_kernel,
        grid=(NDP,),
        in_specs=[
            pl.BlockSpec((OWN, TOK), lambda g: (g, 0), memory_space=pltpu.SMEM),
            pl.BlockSpec((ROWS, TOK), lambda g: (0, 0)),
        ],
        out_specs=pl.BlockSpec((1, OWN, CAP, TOK), lambda g: (g, 0, 0, 0)),
        out_shape=shape((NDP, OWN, CAP, TOK), BF16),
        scratch_shapes=[
            pltpu.VMEM((ROWS, TOK), F32),
            pltpu.VMEM((OWN * CAP, TOK), F32),
        ],
        compiler_params=PARAMS,
        name="gather_rows",
    )(row, table)


DOT_OWN = 8


def dots_kernel(part, *refs):
    rows_ref, value_ref = refs[:2]
    out_ref = refs[-1]
    place = lax.broadcasted_iota(jnp.int32, (CAP, TOK), 0)
    lane = lax.broadcasted_iota(jnp.int32, (CAP, TOK), 1)
    own = place == lane
    made = []
    for t in range(DOT_OWN):
        if part == 1:
            made.append(refs[2][t * PART : (t + 1) * PART, :])
        for k in range(PART):
            product = rows_ref[t, k * CAP : (k + 1) * CAP, :].astype(F32) * value_ref[
                k, t
            ].astype(F32)
            total = jnp.sum(product, axis=1, keepdims=True)
            made.append(jnp.sum(jnp.where(own, total, 0.0), axis=0, keepdims=True))
    out_ref[...] = jnp.concatenate(made, axis=0)


def dots(part, rows, value, earlier=()):
    steps = OWN // DOT_OWN
    count = DOT_OWN * (PART if part == 0 else NDP)
    return pl.pallas_call(
        functools.partial(dots_kernel, part),
        grid=(steps,),
        in_specs=[
            pl.BlockSpec((DOT_OWN, rows.shape[1], TOK), lambda g: (g, 0, 0)),
            pl.BlockSpec((PART, DOT_OWN, CAP, TOK), lambda g: (part, g, 0, 0)),
        ]
        + [pl.BlockSpec((DOT_OWN * PART, TOK), lambda g: (g, 0))] * len(earlier),
        out_specs=pl.BlockSpec((count, TOK), lambda g: (g, 0)),
        out_shape=shape((count * steps, TOK), F32),
        compiler_params=PARAMS,
        name="dots",
    )(rows, value, *earlier)


def scatter_kernel(row_ref, weight_ref, rows_a_ref, rows_b_ref, out_ref, sq_ref, wide_ref, *accs):
    step = pl.program_id(0)

    @pl.when(step == 0)
    def _():
        def clear(i, carry):
            at = pl.multiple_of(i * 64, 64)
            for acc in accs:
                acc[pl.ds(at, 64), :] = jnp.zeros((64, TOK), F32)
            return carry

        lax.fori_loop(0, ROWS // 64, clear, 0)

    columns = jnp.transpose(jnp.concatenate([weight_ref[...]] * (TOK // OWN), axis=0))
    for part, rows_ref in ((0, rows_a_ref), (1, rows_b_ref)):

        @pl.when(step // PART == part)
        def _():
            for t in range(OWN):
                wide_ref[t * CAP : (t + 1) * CAP, :] = (
                    rows_ref[t].astype(F32) * columns[0:CAP, t : t + 1]
                )

    waiting = []
    for t in range(OWN):
        for b in range(0, CAP, BATCH):
            made = []
            for j in range(b, b + BATCH):
                acc = accs[j % ACCS]
                row = row_ref[t, j]
                made.append((acc, row, acc[pl.ds(row, 1), :] + wide_ref[pl.ds(t * CAP + j, 1), :]))
            for acc, row, total in waiting:
                acc[pl.ds(row, 1), :] = total
            waiting = made
    for acc, row, total in waiting:
        acc[pl.ds(row, 1), :] = total

    @pl.when(step == pl.num_programs(0) - 1)
    def _():
        def collect(i, total):
            at = pl.multiple_of(i * 64, 64)
            value = accs[0][pl.ds(at, 64), :]
            for acc in accs[1:]:
                value = value + acc[pl.ds(at, 64), :]
            out_ref[pl.ds(at, 64), :] = value
            square = value * value
            return total + jnp.sum(square.reshape(8, 8, TOK), axis=0)

        sq_ref[...] = lax.fori_loop(0, ROWS // 64, collect, jnp.zeros((8, TOK), F32))


def scatter_rows(row, weight, rows_a, rows_b):
    return pl.pallas_call(
        scatter_kernel,
        grid=(NDP,),
        in_specs=[
            pl.BlockSpec((OWN, TOK), lambda g: (g, 0), memory_space=pltpu.SMEM),
            pl.BlockSpec((OWN, TOK), lambda g: (g, 0)),
            pl.BlockSpec((OWN, CAP, TOK), lambda g: (0, jnp.minimum(g, PART - 1), 0)),
            pl.BlockSpec((OWN, CAP, TOK), lambda g: (0, jnp.maximum(g - PART, 0), 0)),
        ],
        out_specs=vmem(2),
        out_shape=(shape((ROWS, TOK), F32), shape((8, TOK), F32)),
        scratch_shapes=[pltpu.VMEM((OWN * CAP, TOK), F32)]
        + [pltpu.VMEM((ROWS, TOK), F32) for _ in range(ACCS)],
        compiler_params=pltpu.CompilerParams(vmem_limit_bytes=52 * 1024 * 1024),
        name="scatter_rows",
    )(row, weight, rows_a, rows_b)


SCALE_ROWS = 1024


def scale_kernel(factor_ref, value_ref, out_ref):
    out_ref[...] = value_ref[...] * factor_ref[0]


def scaled(factor, value):
    return pl.pallas_call(
        scale_kernel,
        grid=(ROWS // SCALE_ROWS,),
        in_specs=smem() + [pl.BlockSpec((SCALE_ROWS, TOK), lambda g: (g, 0))],
        out_specs=pl.BlockSpec((SCALE_ROWS, TOK), lambda g: (g, 0)),
        out_shape=shape((ROWS, TOK), F32),
        compiler_params=pltpu.CompilerParams(vmem_limit_bytes=60 * 1024 * 1024),
        name="scale",
    )(factor, value)


def dscore_kernel(me_ref, ret_ref, *refs):
    late_refs = refs[:NDP]
    out_ref = refs[NDP]
    owner_id = lax.broadcasted_iota(jnp.int32, (OWN, TOK), 0)
    place_id = lax.broadcasted_iota(jnp.int32, (CAP, TOK), 0)
    row = lax.broadcasted_iota(jnp.int32, (PICKS, TOK), 0)
    for s in range(NDP):
        late_ref = late_refs[s]
        which = source(me_ref[0], s)
        square = jnp.concatenate([ret_ref[:, which, :]] * 4, axis=0)
        columns = jnp.transpose(square)[0:CAP, 0:OWN]
        stacked = jnp.concatenate(pieces(columns), axis=0)
        target = [late_index(late_ref, k, 3) for k in range(PICKS)]
        chosen = jnp.concatenate(
            [
                jnp.where(owner_id == jnp.right_shift(target[k], 7), 1.0, 0.0).astype(BF16)
                for k in range(PICKS)
            ],
            axis=1,
        )
        got = lax.dot_general(stacked, chosen, NN, preferred_element_type=F32)
        got = (got[0:CAP, :] + got[CAP : 2 * CAP, :]) + got[2 * CAP : 3 * CAP, :]
        picked = jnp.concatenate(
            [
                jnp.sum(
                    jnp.where(
                        place_id == jnp.bitwise_and(target[k], TOK - 1),
                        got[:, k * TOK : (k + 1) * TOK],
                        0.0,
                    ),
                    axis=0,
                    keepdims=True,
                )
                for k in range(PICKS)
            ],
            axis=0,
        )
        weight = jnp.concatenate(
            [
                joined(*[late_ref[p : p + 1, k * TOK : (k + 1) * TOK] for p in range(3)])
                for k in range(PICKS)
            ],
            axis=0,
        )
        both = weight * picked
        mean0 = jnp.sum(both[0:4, :], axis=0, keepdims=True)
        mean1 = jnp.sum(both[4:8, :], axis=0, keepdims=True)
        at = pl.multiple_of(which * 8, 8)
        slope = weight * (picked - jnp.where(row < 4, mean0, mean1))
        for d in range(NDP):
            out_ref[d, pl.ds(at, 8), :] = slope


def partial_dscore(me, returned, late):
    return pl.pallas_call(
        dscore_kernel,
        grid=(1,),
        in_specs=smem()
        + vmem(1)
        + [pl.BlockSpec((EXTRA, 4 * HALF), lambda g: (TOK // EXTRA, 0))] * NDP,
        out_specs=vmem(1)[0],
        out_shape=shape((NDP, NDP * PICKS, TOK), F32),
        compiler_params=PARAMS,
        name="dscore",
    )(me, returned, *late)


def key_kernel(me_ref, ds_ref, *refs):
    late_refs = refs[:NDP]
    out_ref = refs[NDP]
    base = me_ref[0] * KEYS
    dscore = []
    for s in range(NDP):
        at = pl.multiple_of(source(me_ref[0], s) * 8, 8)
        total = ds_ref[0, pl.ds(at, 8), :]
        for d in range(1, NDP):
            total = total + ds_ref[d, pl.ds(at, 8), :]
        dscore.append(total)
    key_id = lax.broadcasted_iota(jnp.int32, (KEYS, TOK), 0) + base
    for half in range(2):
        for head in range(2):
            at = head * 2 * HALF + half * HALF
            blocks = []
            for s in range(NDP):
                block = jnp.zeros((KEYS, TOK), F32)
                for k in range(4):
                    slot = head * 4 + k
                    value = dscore[s][slot : slot + 1, :]
                    block = block + jnp.where(
                        key_id == late_index(late_refs[s], slot, TOK + 5 + 2 * half), value, 0.0
                    )
                blocks.append(block)
            weighted = jnp.concatenate(blocks, axis=1)
            query = jnp.concatenate(
                [late_refs[s][0:TOK, at : at + HALF] for s in range(NDP)], axis=0
            )
            stacked = jnp.concatenate(pieces(weighted), axis=0)
            total = lax.dot_general(stacked, query, NN, preferred_element_type=F32)
            total = (total[0:KEYS, :] + total[KEYS : 2 * KEYS, :]) + total[2 * KEYS : 3 * KEYS, :]
            r = half * 4 + head * 2
            out_ref[:, r : r + 2, :] = total.reshape(OWN, 2, HALF)


def key_terms(me, dscore, late):
    return pl.pallas_call(
        key_kernel,
        in_specs=smem() + vmem(1 + NDP),
        out_specs=vmem(1)[0],
        out_shape=shape((OWN, 8, HALF), F32),
        compiler_params=PARAMS,
        name="key_terms",
    )(me, dscore, *late)


def exchange(x, axis):
    return lax.all_to_all(x, axis, 0, 0, tiled=True)


def everyone(x, axis, size):
    return exchange(jnp.broadcast_to(x[None], (size, *x.shape)), axis)


def body(queries, sub_keys, values, slot_first, slot_second, cotangent):
    q = queries.reshape(TOK, 4 * HALF)
    first = slot_first.reshape(TOK, PICKS).T
    second = slot_second.reshape(TOK, PICKS).T
    me = lax.axis_index("dp").astype(jnp.int32).reshape(1)
    outgoing, late = prep(q, sub_keys, first, second, cotangent)
    sent = exchange(outgoing, "dp")
    expanded = expand(0, sent)
    rows_a = exchange(expanded, TABLE)
    expanded = expand(1, sent)
    rows_b = exchange(expanded, TABLE)
    late, _ = lax.optimization_barrier((late, sent))
    late_all = [late] + [
        lax.ppermute(late, "dp", [(i, (i + k) % NDP) for i in range(NDP)])
        for k in range(1, NDP)
    ]
    row, weight = decode(rows_a)
    value_rows = gather_rows(row, values.reshape(ROWS, TOK))
    partial = dots(0, rows_a, value_rows)
    partial = dots(1, rows_b, value_rows, (partial,))
    returned = exchange(partial.reshape(OWN, NDP, TOK), TABLE)
    value_grad, value_sq = scatter_rows(row, weight, rows_a, rows_b)
    slopes = partial_dscore(me, returned, late_all)
    dscore = exchange(slopes, "dp")
    key_grad = key_terms(me, dscore, late_all)
    key_pieces = exchange(key_grad, TABLE)
    key_part = jnp.sum(key_pieces, axis=0)
    local_sq = (jnp.sum(value_sq) + jnp.sum(key_part * key_part)).reshape(1)
    chip_sq = local_sq + lax.ppermute(local_sq, "table_2", [(0, 1), (1, 0)])
    total_sq = jnp.sum(everyone(chip_sq, CHIPS, OWN * NDP // 2))
    clip_factor = jnp.minimum(
        1.0, LIMIT_RATIO * math.sqrt(TOK * OWN * NDP) / jnp.sqrt(total_sq)
    ).reshape(1)
    value_update = scaled(clip_factor, value_grad).reshape(BLK, NSUB, TOK)
    key_update = (clip_factor[0] * key_part).reshape(2, 2, 2, HALF)
    return (value_update, key_update, clip_factor)


def solution(mesh):
    torus = Mesh(
        mesh.devices.reshape(mesh.shape["dp"], 4, 4, 2), ("dp", "table_0", "table_1", "table_2")
    )
    return jax.shard_map(
        body,
        mesh=torus,
        in_specs=(
            P(DP_TABLE, None, None),
            P(),
            P(TABLE, None, "dp"),
            P(DP_TABLE, None, None),
            P(DP_TABLE, None, None),
            P(DP_TABLE, None),
        ),
        out_specs=(P(TABLE, None, "dp"), P(None, None, DP_TABLE, None), P()),
        check_vma=False,
    )
```

```python
import functools
import math

import jax
import jax.numpy as jnp
from jax import lax
from jax.experimental import pallas as pl
from jax.experimental.pallas import tpu as pltpu
from jax.sharding import Mesh
from jax.sharding import PartitionSpec as P


TABLE = ("table_0", "table_1", "table_2")
DP_TABLE = ("dp", "table_0", "table_1", "table_2")
CHIPS = ("dp", "table_0", "table_1")
NSUB = 512
BLK = 16
CAP = 48
OWN = 32
NDP = 8
TOK = 128
PICKS = 8
HALF = 256
KEYS = NSUB // NDP
LISTS = OWN * NDP
PART = NDP // 2
ROWS = BLK * NSUB
RECORDS = 2 * NDP
ACCS = 8
BATCH = 4
EXTRA = 16
F32 = jnp.float32
BF16 = jnp.bfloat16
LIMIT_RATIO = 5.0

NT = (((1,), (1,)), ((), ()))
NN = (((1,), (0,)), ((), ()))

PARAMS = pltpu.CompilerParams(vmem_limit_bytes=20 * 1024 * 1024)
WIDE_PARAMS = pltpu.CompilerParams(vmem_limit_bytes=52 * 1024 * 1024)


def pieces(x):
    high = x.astype(BF16)
    rest = x - high.astype(F32)
    mid = rest.astype(BF16)
    low = (rest - mid.astype(F32)).astype(BF16)
    return high, mid, low


def joined(high, mid, low):
    return (high.astype(F32) + mid.astype(F32)) + low.astype(F32)


def vmem(count):
    return [pl.BlockSpec(memory_space=pltpu.VMEM)] * count


def smem():
    return [pl.BlockSpec(memory_space=pltpu.SMEM)]


def shape(dims, kind):
    return jax.ShapeDtypeStruct(dims, kind)


def prep_kernel(q_ref, keys_ref, first_ref, second_ref, cot_ref, out_ref, late_ref):
    first = first_ref[...]
    second = second_ref[...]
    key_id = lax.broadcasted_iota(jnp.int32, (NSUB, TOK), 0)
    scores = [None] * PICKS
    for half, index in ((0, first), (1, second)):
        for head in range(2):
            at = head * 2 * HALF + half * HALF
            table = lax.dot_general(
                keys_ref[half, head], q_ref[:, at : at + HALF], NT, preferred_element_type=F32
            )
            for k in range(4):
                slot = head * 4 + k
                part = jnp.sum(
                    jnp.where(key_id == index[slot : slot + 1, :], table, 0.0),
                    axis=0,
                    keepdims=True,
                )
                scores[slot] = part if scores[slot] is None else scores[slot] + part
    exps = [jnp.exp(s) for s in scores]
    weights = []
    for head in range(2):
        e = exps[head * 4 : head * 4 + 4]
        total = (e[0] + e[1]) + (e[2] + e[3])
        weights += [x / total for x in e]
    owner = jnp.right_shift(first, 4)
    owner_id = lax.broadcasted_iota(jnp.int32, (OWN, TOK), 0)
    member = [
        jnp.where(owner_id == owner[s : s + 1, :], 1.0, 0.0).astype(F32) for s in range(PICKS)
    ]
    earlier = jnp.where(
        lax.broadcasted_iota(jnp.int32, (TOK, TOK), 0)
        < lax.broadcasted_iota(jnp.int32, (TOK, TOK), 1),
        1.0,
        0.0,
    ).astype(BF16)
    member_all = jnp.concatenate(member, axis=0).astype(BF16)
    ranks = lax.dot_general(member_all, earlier, NN, preferred_element_type=F32)
    base = jnp.zeros((OWN, 1), F32)
    token = lax.broadcasted_iota(jnp.int32, (1, TOK), 1).astype(F32)
    lane_id = lax.broadcasted_iota(jnp.int32, (TOK, TOK), 0)
    planes = [jnp.zeros((OWN, TOK), F32)] * 2
    targets = []
    for s in range(PICKS):
        rank = jnp.sum(
            member[s] * (ranks[s * OWN : (s + 1) * OWN, :] + base), axis=0, keepdims=True
        )
        base = base + jnp.sum(member[s], axis=1, keepdims=True)
        place = rank.astype(jnp.int32)
        row = jnp.bitwise_and(first[s : s + 1, :], BLK - 1) * NSUB + second[s : s + 1, :]
        at_value = lane_id == place
        at_rest = lane_id == place + CAP
        at_token = (
            lane_id == place + 2 * CAP,
            lane_id == jnp.where(place >= TOK - 2 * CAP, place + 4 * CAP - TOK, -1),
        )
        weight = pieces(weights[s])
        parts = (
            (jnp.right_shift(row, 5).astype(F32), jnp.bitwise_and(row, 31).astype(F32)),
            (weight[0].astype(F32), weight[1].astype(F32)),
        )
        chosen = member[s].astype(BF16)
        for p in range(2):
            entry = jnp.where(
                at_value,
                parts[p][0],
                jnp.where(at_rest, parts[p][1], jnp.where(at_token[p], token, 0.0)),
            ).astype(BF16)
            planes[p] = planes[p] + lax.dot_general(
                chosen, entry, NT, preferred_element_type=F32
            )
        targets.append(owner[s : s + 1, :] * TOK + place)
    planes = [plane.astype(BF16) for plane in planes]
    for d in range(NDP):
        out_ref[d, 0:TOK, :] = cot_ref[:, d * TOK : (d + 1) * TOK]
        for p in range(2):
            out_ref[d, TOK + p * OWN : TOK + (p + 1) * OWN, :] = planes[p]
    late_ref[0:TOK, :] = q_ref[...]
    parts = list(pieces(jnp.concatenate(weights, axis=0)))
    for index in (jnp.concatenate(targets, axis=0), first, second):
        parts += [
            jnp.right_shift(index, 6).astype(F32).astype(BF16),
            jnp.bitwise_and(index, 63).astype(F32).astype(BF16),
        ]
    parts = [part.astype(F32) for part in parts]
    parts += [jnp.zeros((PICKS, TOK), F32)] * (EXTRA - len(parts))
    for s in range(PICKS):
        late_ref[TOK : TOK + EXTRA, s * TOK : (s + 1) * TOK] = jnp.concatenate(
            [part[s : s + 1, :] for part in parts], axis=0
        ).astype(BF16)


def prep(q, keys, first, second, cot):
    return pl.pallas_call(
        prep_kernel,
        in_specs=vmem(5),
        out_specs=vmem(2),
        out_shape=(
            shape((NDP, TOK + 2 * OWN, TOK), BF16),
            shape((TOK + EXTRA, 4 * HALF), BF16),
        ),
        compiler_params=WIDE_PARAMS,
        name="prep",
    )(q, keys, first, second, cot)


def late_index(late_ref, slot, part):
    at = slice(slot * TOK, (slot + 1) * TOK)
    high = late_ref[part : part + 1, at].astype(F32).astype(jnp.int32)
    low = late_ref[part + 1 : part + 2, at].astype(F32).astype(jnp.int32)
    return high * 64 + low


def source(me, k):
    return jnp.bitwise_and(me + NDP - k, NDP - 1)


def expand_kernel(part, sent_ref, out_ref, *scratch):
    lane = lax.broadcasted_iota(jnp.int32, (CAP, TOK), 1)
    for k in range(PART):
        s = part * PART + k
        planes = [sent_ref[s, TOK + p * OWN : TOK + (p + 1) * OWN, :].astype(F32) for p in range(2)]
        columns = [jnp.transpose(jnp.concatenate([plane] * 4, axis=0)) for plane in planes]
        token = jnp.concatenate(
            [columns[0][2 * CAP : TOK, :], columns[1][2 * CAP : 5 * CAP - TOK, :]], axis=0
        ).astype(jnp.int32)
        chosen = jnp.concatenate(
            [
                jnp.where(token[:, o : o + 1] == lane, 1.0, 0.0).astype(BF16)
                for o in range(OWN)
            ],
            axis=0,
        )
        out_ref[:, k * CAP : (k + 1) * CAP, :] = (
            lax.dot_general(chosen, sent_ref[s, 0:TOK, :], NN, preferred_element_type=F32)
            .astype(BF16)
            .reshape(OWN, CAP, TOK)
        )
    if part == 0:
        wide_ref = scratch[0]
        for s in range(NDP):
            for p in range(2):
                wide_ref[:, 2 * s + p, :] = sent_ref[
                    s, TOK + p * OWN : TOK + (p + 1) * OWN, :
                ].astype(F32)
        out_ref[:, PART * CAP :, :] = wide_ref[...].astype(BF16)


def expand(part, sent):
    extra = RECORDS if part == 0 else 0
    return pl.pallas_call(
        functools.partial(expand_kernel, part),
        in_specs=vmem(1),
        out_specs=vmem(1)[0],
        out_shape=shape((OWN, PART * CAP + extra, TOK), BF16),
        scratch_shapes=[pltpu.VMEM((OWN, RECORDS, TOK), F32)] if part == 0 else [],
        compiler_params=PARAMS,
        name="expand",
    )(sent)


def decode_kernel(rows_ref, row_ref, weight_ref, wide_ref):
    for t in range(OWN):
        wide_ref[t * RECORDS : (t + 1) * RECORDS, :] = rows_ref[t, PART * CAP :, :].astype(F32)
    for s in range(NDP):
        index = wide_ref[pl.ds(2 * s, OWN, stride=RECORDS), :]
        weight = wide_ref[pl.ds(2 * s + 1, OWN, stride=RECORDS), :]
        at = slice(s * OWN, (s + 1) * OWN)
        row_ref[at, :] = (index * 32.0 + pltpu.roll(index, TOK - CAP, 1)).astype(jnp.int32)
        weight_ref[at, :] = weight + pltpu.roll(weight, TOK - CAP, 1)


def decode(rows):
    return pl.pallas_call(
        decode_kernel,
        in_specs=vmem(1),
        out_specs=vmem(2),
        out_shape=(shape((LISTS, TOK), jnp.int32), shape((LISTS, TOK), F32)),
        scratch_shapes=[pltpu.VMEM((OWN * RECORDS, TOK), F32)],
        compiler_params=PARAMS,
        name="decode",
    )(rows)


def gather_kernel(row_ref, table_ref, out_ref, wide_ref, got_ref):
    @pl.when(pl.program_id(0) == 0)
    def _():
        def widen(i, carry):
            at = pl.multiple_of(i * 256, 256)
            wide_ref[pl.ds(at, 256), :] = table_ref[pl.ds(at, 256), :].astype(F32)
            return carry

        lax.fori_loop(0, ROWS // 256, widen, 0)

    for t in range(OWN):
        for j in range(CAP):
            row = row_ref[t, j]
            got_ref[pl.ds(t * CAP + j, 1), :] = wide_ref[pl.ds(row, 1), :]
    out_ref[...] = got_ref[...].astype(BF16).reshape(1, OWN, CAP, TOK)


def gather_rows(row, table):
    return pl.pallas_call(
        gather_kernel,
        grid=(NDP,),
        in_specs=[
            pl.BlockSpec((OWN, TOK), lambda g: (g, 0), memory_space=pltpu.SMEM),
            pl.BlockSpec((ROWS, TOK), lambda g: (0, 0)),
        ],
        out_specs=pl.BlockSpec((1, OWN, CAP, TOK), lambda g: (g, 0, 0, 0)),
        out_shape=shape((NDP, OWN, CAP, TOK), BF16),
        scratch_shapes=[
            pltpu.VMEM((ROWS, TOK), F32),
            pltpu.VMEM((OWN * CAP, TOK), F32),
        ],
        compiler_params=PARAMS,
        name="gather_rows",
    )(row, table)


DOT_OWN = 8


def dots_kernel(part, *refs):
    rows_ref, value_ref = refs[:2]
    out_ref = refs[-1]
    place = lax.broadcasted_iota(jnp.int32, (CAP, TOK), 0)
    lane = lax.broadcasted_iota(jnp.int32, (CAP, TOK), 1)
    own = place == lane
    made = []
    for t in range(DOT_OWN):
        if part == 1:
            made.append(refs[2][t * PART : (t + 1) * PART, :])
        for k in range(PART):
            product = rows_ref[t, k * CAP : (k + 1) * CAP, :].astype(F32) * value_ref[
                k, t
            ].astype(F32)
            total = jnp.sum(product, axis=1, keepdims=True)
            made.append(jnp.sum(jnp.where(own, total, 0.0), axis=0, keepdims=True))
    out_ref[...] = jnp.concatenate(made, axis=0)


def dots(part, rows, value, earlier=()):
    steps = OWN // DOT_OWN
    count = DOT_OWN * (PART if part == 0 else NDP)
    return pl.pallas_call(
        functools.partial(dots_kernel, part),
        grid=(steps,),
        in_specs=[
            pl.BlockSpec((DOT_OWN, rows.shape[1], TOK), lambda g: (g, 0, 0)),
            pl.BlockSpec((PART, DOT_OWN, CAP, TOK), lambda g: (part, g, 0, 0)),
        ]
        + [pl.BlockSpec((DOT_OWN * PART, TOK), lambda g: (g, 0))] * len(earlier),
        out_specs=pl.BlockSpec((count, TOK), lambda g: (g, 0)),
        out_shape=shape((count * steps, TOK), F32),
        compiler_params=PARAMS if part == 0 else WIDE_PARAMS,
        name="dots",
    )(rows, value, *earlier)


def weigh_kernel(weight_ref, rows_ref, *refs):
    out_ref = refs[-1]
    columns = jnp.transpose(jnp.concatenate([weight_ref[...]] * (TOK // OWN), axis=0))
    for t in range(OWN):
        out_ref[t * CAP : (t + 1) * CAP, :] = (
            rows_ref[t].astype(F32) * columns[0:CAP, t : t + 1]
        )


def weigh(part, weight, rows, earlier=()):
    return pl.pallas_call(
        weigh_kernel,
        grid=(PART,),
        in_specs=[
            pl.BlockSpec((OWN, TOK), lambda g: (part * PART + g, 0)),
            pl.BlockSpec((OWN, CAP, TOK), lambda g: (0, g, 0)),
        ]
        + [pl.BlockSpec(memory_space=pl.ANY)] * len(earlier),
        out_specs=pl.BlockSpec((OWN * CAP, TOK), lambda g: (part * PART + g, 0)),
        out_shape=shape((LISTS * CAP, TOK), F32),
        input_output_aliases={2: 0} if earlier else {},
        compiler_params=WIDE_PARAMS,
        name="weigh",
    )(weight, rows, *earlier)


def scatter_kernel(row_ref, wide_ref, out_ref, sq_ref, *accs):
    step = pl.program_id(0)

    @pl.when(step == 0)
    def _():
        def clear(i, carry):
            at = pl.multiple_of(i * 64, 64)
            for acc in accs:
                acc[pl.ds(at, 64), :] = jnp.zeros((64, TOK), F32)
            return carry

        lax.fori_loop(0, ROWS // 64, clear, 0)

    waiting = []
    for t in range(OWN):
        for b in range(0, CAP, BATCH):
            made = []
            for j in range(b, b + BATCH):
                acc = accs[j % ACCS]
                row = row_ref[t, j]
                made.append((acc, row, acc[pl.ds(row, 1), :] + wide_ref[pl.ds(t * CAP + j, 1), :]))
            for acc, row, total in waiting:
                acc[pl.ds(row, 1), :] = total
            waiting = made
    for acc, row, total in waiting:
        acc[pl.ds(row, 1), :] = total

    @pl.when(step == pl.num_programs(0) - 1)
    def _():
        def collect(i, total):
            at = pl.multiple_of(i * 64, 64)
            value = accs[0][pl.ds(at, 64), :]
            for acc in accs[1:]:
                value = value + acc[pl.ds(at, 64), :]
            out_ref[pl.ds(at, 64), :] = value
            square = value * value
            return total + jnp.sum(square.reshape(8, 8, TOK), axis=0)

        sq_ref[...] = lax.fori_loop(0, ROWS // 64, collect, jnp.zeros((8, TOK), F32))


def scatter_rows(row, wide):
    return pl.pallas_call(
        scatter_kernel,
        grid=(NDP,),
        in_specs=[
            pl.BlockSpec((OWN, TOK), lambda g: (g, 0), memory_space=pltpu.SMEM),
            pl.BlockSpec((OWN * CAP, TOK), lambda g: (g, 0)),
        ],
        out_specs=vmem(2),
        out_shape=(shape((ROWS, TOK), F32), shape((8, TOK), F32)),
        scratch_shapes=[pltpu.VMEM((ROWS, TOK), F32) for _ in range(ACCS)],
        compiler_params=WIDE_PARAMS,
        name="scatter_rows",
    )(row, wide)


def finish_kernel(pieces_ref, sq_ref, part_ref, local_ref):
    part = pieces_ref[0]
    for t in range(1, OWN):
        part = part + pieces_ref[t]
    part_ref[...] = part
    square = part * part
    total = sq_ref[...] + (square[:, 0:TOK] + square[:, TOK:])
    total = jnp.sum(jnp.sum(total, axis=0, keepdims=True), axis=1, keepdims=True)
    local_ref[...] = jnp.broadcast_to(total, (1, TOK))


def finish(key_pieces, value_sq):
    return pl.pallas_call(
        finish_kernel,
        in_specs=vmem(2),
        out_specs=vmem(2),
        out_shape=(shape((8, HALF), F32), shape((1, TOK), F32)),
        compiler_params=PARAMS,
        name="finish",
    )(key_pieces, value_sq)


CHUNKS = 8


def scale_kernel(limit, sums_ref, part_ref, value_ref, out_ref, key_ref, clip_ref, buf, come, go):
    size = ROWS // CHUNKS

    def part_of(ref, i):
        return ref.at[pl.ds(i * size, size), :]

    reads = [
        pltpu.make_async_copy(part_of(value_ref, i), part_of(buf, i), come.at[i])
        for i in range(CHUNKS)
    ]
    writes = [
        pltpu.make_async_copy(part_of(buf, i), part_of(out_ref, i), go.at[i])
        for i in range(CHUNKS)
    ]
    for read in reads:
        read.start()
    total = jnp.sum(sums_ref[...], axis=0, keepdims=True)
    factor = jnp.minimum(1.0, limit / jnp.sqrt(total))
    clip_ref[...] = factor
    keys = part_ref[...] * jnp.concatenate([factor, factor], axis=1)
    for half in range(2):
        for head in range(2):
            r = half * 4 + head * 2
            key_ref[half, head] = keys[r : r + 2, :]
    for i in range(CHUNKS):
        reads[i].wait()
        at = slice(i * size, (i + 1) * size)
        buf[at, :] = buf[at, :] * factor
        writes[i].start()
    for write in writes:
        write.wait()


def scaled(limit, sums, key_part, value):
    return pl.pallas_call(
        functools.partial(scale_kernel, limit),
        in_specs=vmem(2) + [pl.BlockSpec(memory_space=pl.ANY)],
        out_specs=[pl.BlockSpec(memory_space=pl.ANY)] + vmem(2),
        out_shape=(
            shape((ROWS, TOK), F32),
            shape((2, 2, 2, HALF), F32),
            shape((1, TOK), F32),
        ),
        scratch_shapes=[
            pltpu.VMEM((ROWS, TOK), F32),
            pltpu.SemaphoreType.DMA((CHUNKS,)),
            pltpu.SemaphoreType.DMA((CHUNKS,)),
        ],
        compiler_params=WIDE_PARAMS,
        name="scale",
    )(sums, key_part, value)


def dscore_kernel(me_ref, ret_ref, *refs):
    late_refs = refs[:NDP]
    out_ref = refs[NDP]
    owner_id = lax.broadcasted_iota(jnp.int32, (OWN, TOK), 0)
    place_id = lax.broadcasted_iota(jnp.int32, (CAP, TOK), 0)
    row = lax.broadcasted_iota(jnp.int32, (PICKS, TOK), 0)
    for s in range(NDP):
        late_ref = late_refs[s]
        which = source(me_ref[0], s)
        square = jnp.concatenate([ret_ref[:, which, :]] * 4, axis=0)
        columns = jnp.transpose(square)[0:CAP, 0:OWN]
        stacked = jnp.concatenate(pieces(columns), axis=0)
        target = [late_index(late_ref, k, 3) for k in range(PICKS)]
        chosen = jnp.concatenate(
            [
                jnp.where(owner_id == jnp.right_shift(target[k], 7), 1.0, 0.0).astype(BF16)
                for k in range(PICKS)
            ],
            axis=1,
        )
        got = lax.dot_general(stacked, chosen, NN, preferred_element_type=F32)
        got = (got[0:CAP, :] + got[CAP : 2 * CAP, :]) + got[2 * CAP : 3 * CAP, :]
        picked = jnp.concatenate(
            [
                jnp.sum(
                    jnp.where(
                        place_id == jnp.bitwise_and(target[k], TOK - 1),
                        got[:, k * TOK : (k + 1) * TOK],
                        0.0,
                    ),
                    axis=0,
                    keepdims=True,
                )
                for k in range(PICKS)
            ],
            axis=0,
        )
        weight = jnp.concatenate(
            [
                joined(*[late_ref[p : p + 1, k * TOK : (k + 1) * TOK] for p in range(3)])
                for k in range(PICKS)
            ],
            axis=0,
        )
        both = weight * picked
        mean0 = jnp.sum(both[0:4, :], axis=0, keepdims=True)
        mean1 = jnp.sum(both[4:8, :], axis=0, keepdims=True)
        at = pl.multiple_of(which * 8, 8)
        slope = weight * (picked - jnp.where(row < 4, mean0, mean1))
        for d in range(NDP):
            out_ref[d, pl.ds(at, 8), :] = slope


def partial_dscore(me, returned, late):
    return pl.pallas_call(
        dscore_kernel,
        grid=(1,),
        in_specs=smem()
        + vmem(1)
        + [pl.BlockSpec((EXTRA, 4 * HALF), lambda g: (TOK // EXTRA, 0))] * NDP,
        out_specs=vmem(1)[0],
        out_shape=shape((NDP, NDP * PICKS, TOK), F32),
        compiler_params=PARAMS,
        name="dscore",
    )(me, returned, *late)


def key_kernel(me_ref, ds_ref, *refs):
    late_refs = refs[:NDP]
    out_ref = refs[NDP]
    base = me_ref[0] * KEYS
    dscore = []
    for s in range(NDP):
        at = pl.multiple_of(source(me_ref[0], s) * 8, 8)
        total = ds_ref[0, pl.ds(at, 8), :]
        for d in range(1, NDP):
            total = total + ds_ref[d, pl.ds(at, 8), :]
        dscore.append(total)
    key_id = lax.broadcasted_iota(jnp.int32, (KEYS, TOK), 0) + base
    for half in range(2):
        for head in range(2):
            at = head * 2 * HALF + half * HALF
            blocks = []
            for s in range(NDP):
                block = jnp.zeros((KEYS, TOK), F32)
                for k in range(4):
                    slot = head * 4 + k
                    value = dscore[s][slot : slot + 1, :]
                    block = block + jnp.where(
                        key_id == late_index(late_refs[s], slot, TOK + 5 + 2 * half), value, 0.0
                    )
                blocks.append(block)
            weighted = jnp.concatenate(blocks, axis=1)
            query = jnp.concatenate(
                [late_refs[s][0:TOK, at : at + HALF] for s in range(NDP)], axis=0
            )
            stacked = jnp.concatenate(pieces(weighted), axis=0)
            total = lax.dot_general(stacked, query, NN, preferred_element_type=F32)
            total = (total[0:KEYS, :] + total[KEYS : 2 * KEYS, :]) + total[2 * KEYS : 3 * KEYS, :]
            r = half * 4 + head * 2
            out_ref[:, r : r + 2, :] = total.reshape(OWN, 2, HALF)


def key_terms(me, dscore, late):
    return pl.pallas_call(
        key_kernel,
        in_specs=smem() + vmem(1 + NDP),
        out_specs=vmem(1)[0],
        out_shape=shape((OWN, 8, HALF), F32),
        compiler_params=PARAMS,
        name="key_terms",
    )(me, dscore, *late)


def exchange(x, axis):
    return lax.all_to_all(x, axis, 0, 0, tiled=True)


def everyone(x, axis, size):
    return exchange(jnp.broadcast_to(x[None], (size, *x.shape)), axis)


def body(queries, sub_keys, values, slot_first, slot_second, cotangent):
    q = queries.reshape(TOK, 4 * HALF)
    first = slot_first.reshape(TOK, PICKS).T
    second = slot_second.reshape(TOK, PICKS).T
    me = lax.axis_index("dp").astype(jnp.int32).reshape(1)
    outgoing, late = prep(q, sub_keys, first, second, cotangent)
    sent = exchange(outgoing, "dp")
    expanded = expand(0, sent)
    rows_a = exchange(expanded, TABLE)
    expanded = expand(1, sent)
    rows_b = exchange(expanded, TABLE)
    late, _ = lax.optimization_barrier((late, sent))
    late_all = [late] + [
        lax.ppermute(late, "dp", [(i, (i + k) % NDP) for i in range(NDP)])
        for k in range(1, NDP)
    ]
    row, weight = decode(rows_a)
    value_rows = gather_rows(row, values.reshape(ROWS, TOK))
    partial = dots(0, rows_a, value_rows)
    partial = dots(1, rows_b, value_rows, (partial,))
    returned = exchange(partial.reshape(OWN, NDP, TOK), TABLE)
    wide = weigh(0, weight, rows_a)
    wide = weigh(1, weight, rows_b, (wide,))
    value_grad, value_sq = scatter_rows(row, wide)
    slopes = partial_dscore(me, returned, late_all)
    dscore = exchange(slopes, "dp")
    key_grad = key_terms(me, dscore, late_all)
    key_pieces = exchange(key_grad, TABLE)
    key_part, local_sq = finish(key_pieces, value_sq)
    chip_sq = local_sq + lax.ppermute(local_sq, "table_2", [(0, 1), (1, 0)])
    sums = everyone(chip_sq, CHIPS, OWN * NDP // 2)
    limit = LIMIT_RATIO * math.sqrt(TOK * OWN * NDP)
    value_update, key_update, clip = scaled(
        limit, sums.reshape(OWN * NDP // 2, TOK), key_part, value_grad
    )
    return (
        value_update.reshape(BLK, NSUB, TOK),
        key_update,
        clip[0, 0:1],
    )


def solution(mesh):
    torus = Mesh(
        mesh.devices.reshape(mesh.shape["dp"], 4, 4, 2), ("dp", "table_0", "table_1", "table_2")
    )
    return jax.shard_map(
        body,
        mesh=torus,
        in_specs=(
            P(DP_TABLE, None, None),
            P(),
            P(TABLE, None, "dp"),
            P(DP_TABLE, None, None),
            P(DP_TABLE, None, None),
            P(DP_TABLE, None),
        ),
        out_specs=(P(TABLE, None, "dp"), P(None, None, DP_TABLE, None), P()),
        check_vma=False,
    )
```

```python
import functools
import math

import jax
import jax.numpy as jnp
from jax import lax
from jax.experimental import pallas as pl
from jax.experimental.pallas import tpu as pltpu
from jax.sharding import Mesh
from jax.sharding import PartitionSpec as P


TABLE = ("table_0", "table_1", "table_2")
DP_TABLE = ("dp", "table_0", "table_1", "table_2")
CHIPS = ("dp", "table_0", "table_1")
NSUB = 512
BLK = 16
CAP = 48
OWN = 32
NDP = 8
TOK = 128
PICKS = 8
HALF = 256
KEYS = NSUB // NDP
LISTS = OWN * NDP
PART = NDP // 2
ROWS = BLK * NSUB
RECORDS = 2 * NDP
ACCS = 8
BATCH = 4
EXTRA = 16
F32 = jnp.float32
BF16 = jnp.bfloat16
LIMIT_RATIO = 5.0

NT = (((1,), (1,)), ((), ()))
NN = (((1,), (0,)), ((), ()))

PARAMS = pltpu.CompilerParams(vmem_limit_bytes=20 * 1024 * 1024)
WIDE_PARAMS = pltpu.CompilerParams(vmem_limit_bytes=52 * 1024 * 1024)


def pieces(x):
    high = x.astype(BF16)
    rest = x - high.astype(F32)
    mid = rest.astype(BF16)
    low = (rest - mid.astype(F32)).astype(BF16)
    return high, mid, low


def joined(high, mid, low):
    return (high.astype(F32) + mid.astype(F32)) + low.astype(F32)


def vmem(count):
    return [pl.BlockSpec(memory_space=pltpu.VMEM)] * count


def smem():
    return [pl.BlockSpec(memory_space=pltpu.SMEM)]


def shape(dims, kind):
    return jax.ShapeDtypeStruct(dims, kind)


def prep_kernel(q_ref, keys_ref, first_ref, second_ref, cot_ref, out_ref, late_ref):
    first = first_ref[...]
    second = second_ref[...]
    key_id = lax.broadcasted_iota(jnp.int32, (NSUB, TOK), 0)
    scores = [None] * PICKS
    for half, index in ((0, first), (1, second)):
        for head in range(2):
            at = head * 2 * HALF + half * HALF
            table = lax.dot_general(
                keys_ref[half, head], q_ref[:, at : at + HALF], NT, preferred_element_type=F32
            )
            for k in range(4):
                slot = head * 4 + k
                part = jnp.sum(
                    jnp.where(key_id == index[slot : slot + 1, :], table, 0.0),
                    axis=0,
                    keepdims=True,
                )
                scores[slot] = part if scores[slot] is None else scores[slot] + part
    exps = [jnp.exp(s) for s in scores]
    weights = []
    for head in range(2):
        e = exps[head * 4 : head * 4 + 4]
        total = (e[0] + e[1]) + (e[2] + e[3])
        weights += [x / total for x in e]
    owner = jnp.right_shift(first, 4)
    owner_id = lax.broadcasted_iota(jnp.int32, (OWN, TOK), 0)
    member = [
        jnp.where(owner_id == owner[s : s + 1, :], 1.0, 0.0).astype(F32) for s in range(PICKS)
    ]
    earlier = jnp.where(
        lax.broadcasted_iota(jnp.int32, (TOK, TOK), 0)
        < lax.broadcasted_iota(jnp.int32, (TOK, TOK), 1),
        1.0,
        0.0,
    ).astype(BF16)
    member_all = jnp.concatenate(member, axis=0).astype(BF16)
    ranks = lax.dot_general(member_all, earlier, NN, preferred_element_type=F32)
    base = jnp.zeros((OWN, 1), F32)
    token = lax.broadcasted_iota(jnp.int32, (1, TOK), 1).astype(F32)
    lane_id = lax.broadcasted_iota(jnp.int32, (TOK, TOK), 0)
    planes = [jnp.zeros((OWN, TOK), F32)] * 2
    targets = []
    for s in range(PICKS):
        rank = jnp.sum(
            member[s] * (ranks[s * OWN : (s + 1) * OWN, :] + base), axis=0, keepdims=True
        )
        base = base + jnp.sum(member[s], axis=1, keepdims=True)
        place = rank.astype(jnp.int32)
        row = jnp.bitwise_and(first[s : s + 1, :], BLK - 1) * NSUB + second[s : s + 1, :]
        at_value = lane_id == place
        at_rest = lane_id == place + CAP
        at_token = (
            lane_id == place + 2 * CAP,
            lane_id == jnp.where(place >= TOK - 2 * CAP, place + 4 * CAP - TOK, -1),
        )
        weight = pieces(weights[s])
        parts = (
            (jnp.right_shift(row, 5).astype(F32), jnp.bitwise_and(row, 31).astype(F32)),
            (weight[0].astype(F32), weight[1].astype(F32)),
        )
        chosen = member[s].astype(BF16)
        for p in range(2):
            entry = jnp.where(
                at_value,
                parts[p][0],
                jnp.where(at_rest, parts[p][1], jnp.where(at_token[p], token, 0.0)),
            ).astype(BF16)
            planes[p] = planes[p] + lax.dot_general(
                chosen, entry, NT, preferred_element_type=F32
            )
        targets.append(owner[s : s + 1, :] * TOK + place)
    planes = [plane.astype(BF16) for plane in planes]
    for d in range(NDP):
        out_ref[d, 0:TOK, :] = cot_ref[:, d * TOK : (d + 1) * TOK]
        for p in range(2):
            out_ref[d, TOK + p * OWN : TOK + (p + 1) * OWN, :] = planes[p]
    late_ref[0:TOK, :] = q_ref[...]
    parts = list(pieces(jnp.concatenate(weights, axis=0)))
    for index in (jnp.concatenate(targets, axis=0), first, second):
        parts += [
            jnp.right_shift(index, 6).astype(F32).astype(BF16),
            jnp.bitwise_and(index, 63).astype(F32).astype(BF16),
        ]
    parts = [part.astype(F32) for part in parts]
    parts += [jnp.zeros((PICKS, TOK), F32)] * (EXTRA - len(parts))
    for s in range(PICKS):
        late_ref[TOK : TOK + EXTRA, s * TOK : (s + 1) * TOK] = jnp.concatenate(
            [part[s : s + 1, :] for part in parts], axis=0
        ).astype(BF16)


def prep(q, keys, first, second, cot):
    return pl.pallas_call(
        prep_kernel,
        in_specs=vmem(5),
        out_specs=vmem(2),
        out_shape=(
            shape((NDP, TOK + 2 * OWN, TOK), BF16),
            shape((TOK + EXTRA, 4 * HALF), BF16),
        ),
        compiler_params=WIDE_PARAMS,
        name="prep",
    )(q, keys, first, second, cot)


def late_index(late_ref, slot, part):
    at = slice(slot * TOK, (slot + 1) * TOK)
    high = late_ref[part : part + 1, at].astype(F32).astype(jnp.int32)
    low = late_ref[part + 1 : part + 2, at].astype(F32).astype(jnp.int32)
    return high * 64 + low


def source(me, k):
    return jnp.bitwise_and(me + NDP - k, NDP - 1)


def expand_kernel(part, sent_ref, out_ref, *scratch):
    lane = lax.broadcasted_iota(jnp.int32, (CAP, TOK), 1)
    for k in range(PART):
        s = part * PART + k
        planes = [sent_ref[s, TOK + p * OWN : TOK + (p + 1) * OWN, :].astype(F32) for p in range(2)]
        columns = [jnp.transpose(jnp.concatenate([plane] * 4, axis=0)) for plane in planes]
        token = jnp.concatenate(
            [columns[0][2 * CAP : TOK, :], columns[1][2 * CAP : 5 * CAP - TOK, :]], axis=0
        ).astype(jnp.int32)
        chosen = jnp.concatenate(
            [
                jnp.where(token[:, o : o + 1] == lane, 1.0, 0.0).astype(BF16)
                for o in range(OWN)
            ],
            axis=0,
        )
        out_ref[:, k * CAP : (k + 1) * CAP, :] = (
            lax.dot_general(chosen, sent_ref[s, 0:TOK, :], NN, preferred_element_type=F32)
            .astype(BF16)
            .reshape(OWN, CAP, TOK)
        )
    if part == 0:
        wide_ref = scratch[0]
        for s in range(NDP):
            for p in range(2):
                wide_ref[:, 2 * s + p, :] = sent_ref[
                    s, TOK + p * OWN : TOK + (p + 1) * OWN, :
                ].astype(F32)
        out_ref[:, PART * CAP :, :] = wide_ref[...].astype(BF16)


def expand(part, sent):
    extra = RECORDS if part == 0 else 0
    return pl.pallas_call(
        functools.partial(expand_kernel, part),
        in_specs=vmem(1),
        out_specs=vmem(1)[0],
        out_shape=shape((OWN, PART * CAP + extra, TOK), BF16),
        scratch_shapes=[pltpu.VMEM((OWN, RECORDS, TOK), F32)] if part == 0 else [],
        compiler_params=PARAMS,
        name="expand",
    )(sent)


def decode_kernel(rows_ref, row_ref, weight_ref, wide_ref):
    for t in range(OWN):
        wide_ref[t * RECORDS : (t + 1) * RECORDS, :] = rows_ref[t, PART * CAP :, :].astype(F32)
    for s in range(NDP):
        index = wide_ref[pl.ds(2 * s, OWN, stride=RECORDS), :]
        weight = wide_ref[pl.ds(2 * s + 1, OWN, stride=RECORDS), :]
        at = slice(s * OWN, (s + 1) * OWN)
        row_ref[at, :] = (index * 32.0 + pltpu.roll(index, TOK - CAP, 1)).astype(jnp.int32)
        weight_ref[at, :] = weight + pltpu.roll(weight, TOK - CAP, 1)


def decode(rows):
    return pl.pallas_call(
        decode_kernel,
        in_specs=vmem(1),
        out_specs=vmem(2),
        out_shape=(shape((LISTS, TOK), jnp.int32), shape((LISTS, TOK), F32)),
        scratch_shapes=[pltpu.VMEM((OWN * RECORDS, TOK), F32)],
        compiler_params=PARAMS,
        name="decode",
    )(rows)


def gather_kernel(row_ref, table_ref, out_ref, wide_ref, got_ref):
    @pl.when(pl.program_id(0) == 0)
    def _():
        def widen(i, carry):
            at = pl.multiple_of(i * 256, 256)
            wide_ref[pl.ds(at, 256), :] = table_ref[pl.ds(at, 256), :].astype(F32)
            return carry

        lax.fori_loop(0, ROWS // 256, widen, 0)

    for t in range(OWN):
        for j in range(CAP):
            row = row_ref[t, j]
            got_ref[pl.ds(t * CAP + j, 1), :] = wide_ref[pl.ds(row, 1), :]
    out_ref[...] = got_ref[...].astype(BF16).reshape(1, OWN, CAP, TOK)


def gather_rows(row, table):
    return pl.pallas_call(
        gather_kernel,
        grid=(NDP,),
        in_specs=[
            pl.BlockSpec((OWN, TOK), lambda g: (g, 0), memory_space=pltpu.SMEM),
            pl.BlockSpec((ROWS, TOK), lambda g: (0, 0)),
        ],
        out_specs=pl.BlockSpec((1, OWN, CAP, TOK), lambda g: (g, 0, 0, 0)),
        out_shape=shape((NDP, OWN, CAP, TOK), BF16),
        scratch_shapes=[
            pltpu.VMEM((ROWS, TOK), F32),
            pltpu.VMEM((OWN * CAP, TOK), F32),
        ],
        compiler_params=PARAMS,
        name="gather_rows",
    )(row, table)


DOT_OWN = 8


def dots_kernel(part, *refs):
    rows_ref, value_ref = refs[:2]
    out_ref = refs[-1]
    place = lax.broadcasted_iota(jnp.int32, (CAP, TOK), 0)
    lane = lax.broadcasted_iota(jnp.int32, (CAP, TOK), 1)
    own = place == lane
    made = []
    for t in range(DOT_OWN):
        if part == 1:
            made.append(refs[2][t * PART : (t + 1) * PART, :])
        for k in range(PART):
            product = rows_ref[t, k * CAP : (k + 1) * CAP, :].astype(F32) * value_ref[
                k, t
            ].astype(F32)
            total = jnp.sum(product, axis=1, keepdims=True)
            made.append(jnp.sum(jnp.where(own, total, 0.0), axis=0, keepdims=True))
    out_ref[...] = jnp.concatenate(made, axis=0)


def dots(part, rows, value, earlier=()):
    steps = OWN // DOT_OWN
    count = DOT_OWN * (PART if part == 0 else NDP)
    return pl.pallas_call(
        functools.partial(dots_kernel, part),
        grid=(steps,),
        in_specs=[
            pl.BlockSpec((DOT_OWN, rows.shape[1], TOK), lambda g: (g, 0, 0)),
            pl.BlockSpec((PART, DOT_OWN, CAP, TOK), lambda g: (part, g, 0, 0)),
        ]
        + [pl.BlockSpec((DOT_OWN * PART, TOK), lambda g: (g, 0))] * len(earlier),
        out_specs=pl.BlockSpec((count, TOK), lambda g: (g, 0)),
        out_shape=shape((count * steps, TOK), F32),
        compiler_params=PARAMS,
        name="dots",
    )(rows, value, *earlier)


def weigh_kernel(weight_ref, rows_ref, *refs):
    out_ref = refs[-1]
    columns = jnp.transpose(jnp.concatenate([weight_ref[...]] * (TOK // OWN), axis=0))
    for t in range(OWN):
        out_ref[t * CAP : (t + 1) * CAP, :] = (
            rows_ref[t].astype(F32) * columns[0:CAP, t : t + 1]
        )


def weigh(part, weight, rows, earlier=()):
    return pl.pallas_call(
        weigh_kernel,
        grid=(PART,),
        in_specs=[
            pl.BlockSpec((OWN, TOK), lambda g: (part * PART + g, 0)),
            pl.BlockSpec((OWN, CAP, TOK), lambda g: (0, g, 0)),
        ]
        + [pl.BlockSpec(memory_space=pl.ANY)] * len(earlier),
        out_specs=pl.BlockSpec((OWN * CAP, TOK), lambda g: (part * PART + g, 0)),
        out_shape=shape((LISTS * CAP, TOK), F32),
        input_output_aliases={2: 0} if earlier else {},
        compiler_params=WIDE_PARAMS,
        name="weigh",
    )(weight, rows, *earlier)


def scatter_kernel(row_ref, wide_ref, out_ref, sq_ref, even_ref, odd_ref, come, *accs):
    step = pl.program_id(0)
    tables = (even_ref, odd_ref)

    def fetch(which, block):
        at = pl.multiple_of((block * 2 + which) * OWN, OWN)
        return pltpu.make_async_copy(
            row_ref.at[pl.ds(at, OWN), :], tables[which], come.at[which]
        )

    @pl.when(step == 0)
    def _():
        fetch(0, step).start()
        fetch(1, step).start()

        def clear(i, carry):
            at = pl.multiple_of(i * 64, 64)
            for acc in accs:
                acc[pl.ds(at, 64), :] = jnp.zeros((64, TOK), F32)
            return carry

        lax.fori_loop(0, ROWS // 64, clear, 0)

    for which in range(2):
        fetch(which, step).wait()
        waiting = []
        for t in range(OWN):
            for b in range(0, CAP, BATCH):
                made = []
                for j in range(b, b + BATCH):
                    acc = accs[j % ACCS]
                    row = tables[which][t, j]
                    at = (which * OWN + t) * CAP + j
                    made.append((acc, row, acc[pl.ds(row, 1), :] + wide_ref[at : at + 1, :]))
                for acc, row, total in waiting:
                    acc[pl.ds(row, 1), :] = total
                waiting = made
        for acc, row, total in waiting:
            acc[pl.ds(row, 1), :] = total

        @pl.when(step < pl.num_programs(0) - 1)
        def _():
            fetch(which, step + 1).start()

    @pl.when(step == pl.num_programs(0) - 1)
    def _():
        def collect(i, total):
            at = pl.multiple_of(i * 64, 64)
            value = accs[0][pl.ds(at, 64), :]
            for acc in accs[1:]:
                value = value + acc[pl.ds(at, 64), :]
            out_ref[pl.ds(at, 64), :] = value
            square = value * value
            return total + jnp.sum(square.reshape(8, 8, TOK), axis=0)

        sq_ref[...] = lax.fori_loop(0, ROWS // 64, collect, jnp.zeros((8, TOK), F32))


def scatter_rows(row, wide):
    return pl.pallas_call(
        scatter_kernel,
        grid=(NDP // 2,),
        in_specs=[
            pl.BlockSpec(memory_space=pltpu.HBM),
            pl.BlockSpec((2 * OWN * CAP, TOK), lambda g: (g, 0)),
        ],
        out_specs=vmem(2),
        out_shape=(shape((ROWS, TOK), F32), shape((8, TOK), F32)),
        scratch_shapes=[
            pltpu.SMEM((OWN, TOK), jnp.int32),
            pltpu.SMEM((OWN, TOK), jnp.int32),
            pltpu.SemaphoreType.DMA((2,)),
        ]
        + [pltpu.VMEM((ROWS, TOK), F32) for _ in range(ACCS)],
        compiler_params=WIDE_PARAMS,
        name="scatter_rows",
    )(row, wide)


def finish_kernel(pieces_ref, sq_ref, part_ref, local_ref):
    part = pieces_ref[0]
    for t in range(1, OWN):
        part = part + pieces_ref[t]
    part_ref[...] = part
    square = part * part
    total = sq_ref[...] + (square[:, 0:TOK] + square[:, TOK:])
    total = jnp.sum(jnp.sum(total, axis=0, keepdims=True), axis=1, keepdims=True)
    local_ref[...] = jnp.broadcast_to(total, (1, TOK))


def finish(key_pieces, value_sq):
    return pl.pallas_call(
        finish_kernel,
        in_specs=vmem(2),
        out_specs=vmem(2),
        out_shape=(shape((8, HALF), F32), shape((1, TOK), F32)),
        compiler_params=PARAMS,
        name="finish",
    )(key_pieces, value_sq)


CHUNKS = 8


def scale_kernel(limit, sums_ref, part_ref, value_ref, out_ref, key_ref, clip_ref, buf, come, go):
    size = ROWS // CHUNKS

    def part_of(ref, i):
        return ref.at[pl.ds(i * size, size), :]

    reads = [
        pltpu.make_async_copy(part_of(value_ref, i), part_of(buf, i), come.at[i])
        for i in range(CHUNKS)
    ]
    writes = [
        pltpu.make_async_copy(part_of(buf, i), part_of(out_ref, i), go.at[i])
        for i in range(CHUNKS)
    ]
    for read in reads:
        read.start()
    total = jnp.sum(sums_ref[...], axis=0, keepdims=True)
    factor = jnp.minimum(1.0, limit / jnp.sqrt(total))
    clip_ref[...] = factor
    keys = part_ref[...] * jnp.concatenate([factor, factor], axis=1)
    for half in range(2):
        for head in range(2):
            r = half * 4 + head * 2
            key_ref[half, head] = keys[r : r + 2, :]
    for i in range(CHUNKS):
        reads[i].wait()
        at = slice(i * size, (i + 1) * size)
        buf[at, :] = buf[at, :] * factor
        writes[i].start()
    for write in writes:
        write.wait()


def scaled(limit, sums, key_part, value):
    return pl.pallas_call(
        functools.partial(scale_kernel, limit),
        in_specs=vmem(2) + [pl.BlockSpec(memory_space=pl.ANY)],
        out_specs=[pl.BlockSpec(memory_space=pl.ANY)] + vmem(2),
        out_shape=(
            shape((ROWS, TOK), F32),
            shape((2, 2, 2, HALF), F32),
            shape((1, TOK), F32),
        ),
        scratch_shapes=[
            pltpu.VMEM((ROWS, TOK), F32),
            pltpu.SemaphoreType.DMA((CHUNKS,)),
            pltpu.SemaphoreType.DMA((CHUNKS,)),
        ],
        compiler_params=WIDE_PARAMS,
        name="scale",
    )(sums, key_part, value)


def dscore_kernel(me_ref, ret_ref, *refs):
    late_refs = refs[:NDP]
    out_ref = refs[NDP]
    owner_id = lax.broadcasted_iota(jnp.int32, (OWN, TOK), 0)
    place_id = lax.broadcasted_iota(jnp.int32, (CAP, TOK), 0)
    row = lax.broadcasted_iota(jnp.int32, (PICKS, TOK), 0)
    for s in range(NDP):
        late_ref = late_refs[s]
        which = source(me_ref[0], s)
        square = jnp.concatenate([ret_ref[:, which, :]] * 4, axis=0)
        columns = jnp.transpose(square)[0:CAP, 0:OWN]
        stacked = jnp.concatenate(pieces(columns), axis=0)
        target = [late_index(late_ref, k, 3) for k in range(PICKS)]
        chosen = jnp.concatenate(
            [
                jnp.where(owner_id == jnp.right_shift(target[k], 7), 1.0, 0.0).astype(BF16)
                for k in range(PICKS)
            ],
            axis=1,
        )
        got = lax.dot_general(stacked, chosen, NN, preferred_element_type=F32)
        got = (got[0:CAP, :] + got[CAP : 2 * CAP, :]) + got[2 * CAP : 3 * CAP, :]
        picked = jnp.concatenate(
            [
                jnp.sum(
                    jnp.where(
                        place_id == jnp.bitwise_and(target[k], TOK - 1),
                        got[:, k * TOK : (k + 1) * TOK],
                        0.0,
                    ),
                    axis=0,
                    keepdims=True,
                )
                for k in range(PICKS)
            ],
            axis=0,
        )
        weight = jnp.concatenate(
            [
                joined(*[late_ref[p : p + 1, k * TOK : (k + 1) * TOK] for p in range(3)])
                for k in range(PICKS)
            ],
            axis=0,
        )
        both = weight * picked
        mean0 = jnp.sum(both[0:4, :], axis=0, keepdims=True)
        mean1 = jnp.sum(both[4:8, :], axis=0, keepdims=True)
        at = pl.multiple_of(which * 8, 8)
        slope = weight * (picked - jnp.where(row < 4, mean0, mean1))
        for d in range(NDP):
            out_ref[d, pl.ds(at, 8), :] = slope


def partial_dscore(me, returned, late):
    return pl.pallas_call(
        dscore_kernel,
        grid=(1,),
        in_specs=smem()
        + vmem(1)
        + [pl.BlockSpec((EXTRA, 4 * HALF), lambda g: (TOK // EXTRA, 0))] * NDP,
        out_specs=vmem(1)[0],
        out_shape=shape((NDP, NDP * PICKS, TOK), F32),
        compiler_params=PARAMS,
        name="dscore",
    )(me, returned, *late)


def key_kernel(me_ref, ds_ref, *refs):
    late_refs = refs[:NDP]
    out_ref = refs[NDP]
    base = me_ref[0] * KEYS
    dscore = []
    for s in range(NDP):
        at = pl.multiple_of(source(me_ref[0], s) * 8, 8)
        total = ds_ref[0, pl.ds(at, 8), :]
        for d in range(1, NDP):
            total = total + ds_ref[d, pl.ds(at, 8), :]
        dscore.append(total)
    key_id = lax.broadcasted_iota(jnp.int32, (KEYS, TOK), 0) + base
    for half in range(2):
        for head in range(2):
            at = head * 2 * HALF + half * HALF
            blocks = []
            for s in range(NDP):
                block = jnp.zeros((KEYS, TOK), F32)
                for k in range(4):
                    slot = head * 4 + k
                    value = dscore[s][slot : slot + 1, :]
                    block = block + jnp.where(
                        key_id == late_index(late_refs[s], slot, TOK + 5 + 2 * half), value, 0.0
                    )
                blocks.append(block)
            weighted = jnp.concatenate(blocks, axis=1)
            query = jnp.concatenate(
                [late_refs[s][0:TOK, at : at + HALF] for s in range(NDP)], axis=0
            )
            stacked = jnp.concatenate(pieces(weighted), axis=0)
            total = lax.dot_general(stacked, query, NN, preferred_element_type=F32)
            total = (total[0:KEYS, :] + total[KEYS : 2 * KEYS, :]) + total[2 * KEYS : 3 * KEYS, :]
            r = half * 4 + head * 2
            out_ref[:, r : r + 2, :] = total.reshape(OWN, 2, HALF)


def key_terms(me, dscore, late):
    return pl.pallas_call(
        key_kernel,
        in_specs=smem() + vmem(1 + NDP),
        out_specs=vmem(1)[0],
        out_shape=shape((OWN, 8, HALF), F32),
        compiler_params=PARAMS,
        name="key_terms",
    )(me, dscore, *late)


def exchange(x, axis):
    return lax.all_to_all(x, axis, 0, 0, tiled=True)


def everyone(x, axis, size):
    return exchange(jnp.broadcast_to(x[None], (size, *x.shape)), axis)


def body(queries, sub_keys, values, slot_first, slot_second, cotangent):
    q = queries.reshape(TOK, 4 * HALF)
    first = slot_first.reshape(TOK, PICKS).T
    second = slot_second.reshape(TOK, PICKS).T
    me = lax.axis_index("dp").astype(jnp.int32).reshape(1)
    outgoing, late = prep(q, sub_keys, first, second, cotangent)
    sent = exchange(outgoing, "dp")
    expanded = expand(0, sent)
    rows_a = exchange(expanded, TABLE)
    expanded = expand(1, sent)
    rows_b = exchange(expanded, TABLE)
    late, _ = lax.optimization_barrier((late, sent))
    late_all = [late] + [
        lax.ppermute(late, "dp", [(i, (i + k) % NDP) for i in range(NDP)])
        for k in range(1, NDP)
    ]
    row, weight = decode(rows_a)
    value_rows = gather_rows(row, values.reshape(ROWS, TOK))
    partial = dots(0, rows_a, value_rows)
    partial = dots(1, rows_b, value_rows, (partial,))
    returned = exchange(partial.reshape(OWN, NDP, TOK), TABLE)
    wide = weigh(0, weight, rows_a)
    wide = weigh(1, weight, rows_b, (wide,))
    value_grad, value_sq = scatter_rows(row, wide)
    slopes = partial_dscore(me, returned, late_all)
    dscore = exchange(slopes, "dp")
    key_grad = key_terms(me, dscore, late_all)
    key_pieces = exchange(key_grad, TABLE)
    key_part, local_sq = finish(key_pieces, value_sq)
    chip_sq = local_sq + lax.ppermute(local_sq, "table_2", [(0, 1), (1, 0)])
    sums = everyone(chip_sq, CHIPS, OWN * NDP // 2)
    limit = LIMIT_RATIO * math.sqrt(TOK * OWN * NDP)
    value_update, key_update, clip = scaled(
        limit, sums.reshape(OWN * NDP // 2, TOK), key_part, value_grad
    )
    return (
        value_update.reshape(BLK, NSUB, TOK),
        key_update,
        clip[0, 0:1],
    )


def solution(mesh):
    torus = Mesh(
        mesh.devices.reshape(mesh.shape["dp"], 4, 4, 2), ("dp", "table_0", "table_1", "table_2")
    )
    return jax.shard_map(
        body,
        mesh=torus,
        in_specs=(
            P(DP_TABLE, None, None),
            P(),
            P(TABLE, None, "dp"),
            P(DP_TABLE, None, None),
            P(DP_TABLE, None, None),
            P(DP_TABLE, None),
        ),
        out_specs=(P(TABLE, None, "dp"), P(None, None, DP_TABLE, None), P()),
        check_vma=False,
    )
```

```python
import functools
import math

import jax
import jax.numpy as jnp
from jax import lax
from jax.experimental import pallas as pl
from jax.experimental.pallas import tpu as pltpu
from jax.sharding import Mesh
from jax.sharding import PartitionSpec as P


TABLE = ("table_0", "table_1", "table_2")
DP_TABLE = ("dp", "table_0", "table_1", "table_2")
CHIPS = ("dp", "table_0", "table_1")
NSUB = 512
BLK = 16
CAP = 48
OWN = 32
NDP = 8
TOK = 128
PICKS = 8
HALF = 256
KEYS = NSUB // NDP
LISTS = OWN * NDP
PART = NDP // 2
ROWS = BLK * NSUB
RECORDS = 2 * NDP
ACCS = 8
BATCH = 4
EXTRA = 16
CHUNKS = 8
F32 = jnp.float32
BF16 = jnp.bfloat16
LIMIT_RATIO = 5.0

NT = (((1,), (1,)), ((), ()))
NN = (((1,), (0,)), ((), ()))

PARAMS = pltpu.CompilerParams(vmem_limit_bytes=20 * 1024 * 1024)
WIDE_PARAMS = pltpu.CompilerParams(vmem_limit_bytes=52 * 1024 * 1024)


def pieces(x):
    high = x.astype(BF16)
    rest = x - high.astype(F32)
    mid = rest.astype(BF16)
    low = (rest - mid.astype(F32)).astype(BF16)
    return high, mid, low


def joined(high, mid, low):
    return (high.astype(F32) + mid.astype(F32)) + low.astype(F32)


def vmem(count):
    return [pl.BlockSpec(memory_space=pltpu.VMEM)] * count


def smem():
    return [pl.BlockSpec(memory_space=pltpu.SMEM)]


def shape(dims, kind):
    return jax.ShapeDtypeStruct(dims, kind)


def prep_kernel(q_ref, keys_ref, first_ref, second_ref, cot_ref, out_ref, late_ref):
    first = first_ref[...]
    second = second_ref[...]
    key_id = lax.broadcasted_iota(jnp.int32, (NSUB, TOK), 0)
    scores = [None] * PICKS
    for half, index in ((0, first), (1, second)):
        for head in range(2):
            at = head * 2 * HALF + half * HALF
            table = lax.dot_general(
                keys_ref[half, head], q_ref[:, at : at + HALF], NT, preferred_element_type=F32
            )
            for k in range(4):
                slot = head * 4 + k
                part = jnp.sum(
                    jnp.where(key_id == index[slot : slot + 1, :], table, 0.0),
                    axis=0,
                    keepdims=True,
                )
                scores[slot] = part if scores[slot] is None else scores[slot] + part
    exps = [jnp.exp(s) for s in scores]
    weights = []
    for head in range(2):
        e = exps[head * 4 : head * 4 + 4]
        total = (e[0] + e[1]) + (e[2] + e[3])
        weights += [x / total for x in e]
    owner = jnp.right_shift(first, 4)
    owner_id = lax.broadcasted_iota(jnp.int32, (OWN, TOK), 0)
    member = [
        jnp.where(owner_id == owner[s : s + 1, :], 1.0, 0.0).astype(F32) for s in range(PICKS)
    ]
    earlier = jnp.where(
        lax.broadcasted_iota(jnp.int32, (TOK, TOK), 0)
        < lax.broadcasted_iota(jnp.int32, (TOK, TOK), 1),
        1.0,
        0.0,
    ).astype(BF16)
    member_all = jnp.concatenate(member, axis=0).astype(BF16)
    ranks = lax.dot_general(member_all, earlier, NN, preferred_element_type=F32)
    base = jnp.zeros((OWN, 1), F32)
    token = lax.broadcasted_iota(jnp.int32, (1, TOK), 1).astype(F32)
    lane_id = lax.broadcasted_iota(jnp.int32, (TOK, TOK), 0)
    planes = [jnp.zeros((OWN, TOK), F32)] * 2
    targets = []
    for s in range(PICKS):
        rank = jnp.sum(
            member[s] * (ranks[s * OWN : (s + 1) * OWN, :] + base), axis=0, keepdims=True
        )
        base = base + jnp.sum(member[s], axis=1, keepdims=True)
        place = rank.astype(jnp.int32)
        row = jnp.bitwise_and(first[s : s + 1, :], BLK - 1) * NSUB + second[s : s + 1, :]
        at_value = lane_id == place
        at_rest = lane_id == place + CAP
        at_token = (
            lane_id == place + 2 * CAP,
            lane_id == jnp.where(place >= TOK - 2 * CAP, place + 4 * CAP - TOK, -1),
        )
        weight = pieces(weights[s])
        parts = (
            (jnp.right_shift(row, 5).astype(F32), jnp.bitwise_and(row, 31).astype(F32)),
            (weight[0].astype(F32), weight[1].astype(F32)),
        )
        chosen = member[s].astype(BF16)
        for p in range(2):
            entry = jnp.where(
                at_value,
                parts[p][0],
                jnp.where(at_rest, parts[p][1], jnp.where(at_token[p], token, 0.0)),
            ).astype(BF16)
            planes[p] = planes[p] + lax.dot_general(
                chosen, entry, NT, preferred_element_type=F32
            )
        targets.append(owner[s : s + 1, :] * TOK + place)
    planes = [plane.astype(BF16) for plane in planes]
    for d in range(NDP):
        out_ref[d, 0:TOK, :] = cot_ref[:, d * TOK : (d + 1) * TOK]
        for p in range(2):
            out_ref[d, TOK + p * OWN : TOK + (p + 1) * OWN, :] = planes[p]
    late_ref[0:TOK, :] = q_ref[...]
    parts = list(pieces(jnp.concatenate(weights, axis=0)))
    for index in (jnp.concatenate(targets, axis=0), first, second):
        parts += [
            jnp.right_shift(index, 6).astype(F32).astype(BF16),
            jnp.bitwise_and(index, 63).astype(F32).astype(BF16),
        ]
    parts = [part.astype(F32) for part in parts]
    parts += [jnp.zeros((PICKS, TOK), F32)] * (EXTRA - len(parts))
    for s in range(PICKS):
        late_ref[TOK : TOK + EXTRA, s * TOK : (s + 1) * TOK] = jnp.concatenate(
            [part[s : s + 1, :] for part in parts], axis=0
        ).astype(BF16)


def prep(q, keys, first, second, cot):
    return pl.pallas_call(
        prep_kernel,
        in_specs=vmem(5),
        out_specs=vmem(2),
        out_shape=(
            shape((NDP, TOK + 2 * OWN, TOK), BF16),
            shape((TOK + EXTRA, 4 * HALF), BF16),
        ),
        compiler_params=WIDE_PARAMS,
        name="prep",
    )(q, keys, first, second, cot)


def late_index(late_ref, slot, part):
    at = slice(slot * TOK, (slot + 1) * TOK)
    high = late_ref[part : part + 1, at].astype(F32).astype(jnp.int32)
    low = late_ref[part + 1 : part + 2, at].astype(F32).astype(jnp.int32)
    return high * 64 + low


def source(me, k):
    return jnp.bitwise_and(me + NDP - k, NDP - 1)


def expand_kernel(part, sent_ref, out_ref, *scratch):
    lane = lax.broadcasted_iota(jnp.int32, (CAP, TOK), 1)
    for k in range(PART):
        s = part * PART + k
        planes = [sent_ref[s, TOK + p * OWN : TOK + (p + 1) * OWN, :].astype(F32) for p in range(2)]
        columns = [jnp.transpose(jnp.concatenate([plane] * 4, axis=0)) for plane in planes]
        token = jnp.concatenate(
            [columns[0][2 * CAP : TOK, :], columns[1][2 * CAP : 5 * CAP - TOK, :]], axis=0
        ).astype(jnp.int32)
        chosen = jnp.concatenate(
            [
                jnp.where(token[:, o : o + 1] == lane, 1.0, 0.0).astype(BF16)
                for o in range(OWN)
            ],
            axis=0,
        )
        out_ref[:, k * CAP : (k + 1) * CAP, :] = (
            lax.dot_general(chosen, sent_ref[s, 0:TOK, :], NN, preferred_element_type=F32)
            .astype(BF16)
            .reshape(OWN, CAP, TOK)
        )
    if part == 0:
        wide_ref = scratch[0]
        for s in range(NDP):
            for p in range(2):
                wide_ref[:, 2 * s + p, :] = sent_ref[
                    s, TOK + p * OWN : TOK + (p + 1) * OWN, :
                ].astype(F32)
        out_ref[:, PART * CAP :, :] = wide_ref[...].astype(BF16)


def expand(part, sent):
    extra = RECORDS if part == 0 else 0
    return pl.pallas_call(
        functools.partial(expand_kernel, part),
        in_specs=vmem(1),
        out_specs=vmem(1)[0],
        out_shape=shape((OWN, PART * CAP + extra, TOK), BF16),
        scratch_shapes=[pltpu.VMEM((OWN, RECORDS, TOK), F32)] if part == 0 else [],
        compiler_params=PARAMS,
        name="expand",
    )(sent)


def decode_kernel(rows_ref, row_ref, weight_ref, wide_ref):
    for t in range(OWN):
        wide_ref[t * RECORDS : (t + 1) * RECORDS, :] = rows_ref[t, PART * CAP :, :].astype(F32)
    for s in range(NDP):
        index = wide_ref[pl.ds(2 * s, OWN, stride=RECORDS), :]
        weight = wide_ref[pl.ds(2 * s + 1, OWN, stride=RECORDS), :]
        at = slice(s * OWN, (s + 1) * OWN)
        row_ref[at, :] = (index * 32.0 + pltpu.roll(index, TOK - CAP, 1)).astype(jnp.int32)
        weight_ref[at, :] = weight + pltpu.roll(weight, TOK - CAP, 1)


def decode(rows):
    return pl.pallas_call(
        decode_kernel,
        in_specs=vmem(1),
        out_specs=vmem(2),
        out_shape=(shape((LISTS, TOK), jnp.int32), shape((LISTS, TOK), F32)),
        scratch_shapes=[pltpu.VMEM((OWN * RECORDS, TOK), F32)],
        compiler_params=PARAMS,
        name="decode",
    )(rows)


def gather_kernel(row_ref, table_ref, out_ref, wide_ref, got_ref):
    @pl.when(pl.program_id(0) == 0)
    def _():
        def widen(i, carry):
            at = pl.multiple_of(i * 256, 256)
            wide_ref[pl.ds(at, 256), :] = table_ref[pl.ds(at, 256), :].astype(F32)
            return carry

        lax.fori_loop(0, ROWS // 256, widen, 0)

    for t in range(OWN):
        for j in range(CAP):
            row = row_ref[t, j]
            got_ref[pl.ds(t * CAP + j, 1), :] = wide_ref[pl.ds(row, 1), :]
    out_ref[...] = got_ref[...].astype(BF16).reshape(1, OWN, CAP, TOK)


def gather_rows(row, table):
    return pl.pallas_call(
        gather_kernel,
        grid=(NDP,),
        in_specs=[
            pl.BlockSpec((OWN, TOK), lambda g: (g, 0), memory_space=pltpu.SMEM),
            pl.BlockSpec((ROWS, TOK), lambda g: (0, 0)),
        ],
        out_specs=pl.BlockSpec((1, OWN, CAP, TOK), lambda g: (g, 0, 0, 0)),
        out_shape=shape((NDP, OWN, CAP, TOK), BF16),
        scratch_shapes=[
            pltpu.VMEM((ROWS, TOK), F32),
            pltpu.VMEM((OWN * CAP, TOK), F32),
        ],
        compiler_params=PARAMS,
        name="gather_rows",
    )(row, table)


DOT_OWN = 8


def dots_kernel(part, *refs):
    rows_ref, value_ref = refs[:2]
    out_ref = refs[-1]
    place = lax.broadcasted_iota(jnp.int32, (CAP, TOK), 0)
    lane = lax.broadcasted_iota(jnp.int32, (CAP, TOK), 1)
    own = place == lane
    made = []
    for t in range(DOT_OWN):
        if part == 1:
            made.append(refs[2][t * PART : (t + 1) * PART, :])
        for k in range(PART):
            product = rows_ref[t, k * CAP : (k + 1) * CAP, :].astype(F32) * value_ref[
                k, t
            ].astype(F32)
            total = jnp.sum(product, axis=1, keepdims=True)
            made.append(jnp.sum(jnp.where(own, total, 0.0), axis=0, keepdims=True))
    out_ref[...] = jnp.concatenate(made, axis=0)


def dots(part, rows, value, earlier=()):
    steps = OWN // DOT_OWN
    count = DOT_OWN * (PART if part == 0 else NDP)
    return pl.pallas_call(
        functools.partial(dots_kernel, part),
        grid=(steps,),
        in_specs=[
            pl.BlockSpec((DOT_OWN, rows.shape[1], TOK), lambda g: (g, 0, 0)),
            pl.BlockSpec((PART, DOT_OWN, CAP, TOK), lambda g: (part, g, 0, 0)),
        ]
        + [pl.BlockSpec((DOT_OWN * PART, TOK), lambda g: (g, 0))] * len(earlier),
        out_specs=pl.BlockSpec((count, TOK), lambda g: (g, 0)),
        out_shape=shape((count * steps, TOK), F32),
        compiler_params=PARAMS,
        name="dots",
    )(rows, value, *earlier)


def weigh_kernel(weight_ref, rows_ref, *refs):
    out_ref = refs[-1]
    columns = jnp.transpose(jnp.concatenate([weight_ref[...]] * (TOK // OWN), axis=0))
    for t in range(OWN):
        out_ref[t * CAP : (t + 1) * CAP, :] = (
            rows_ref[t].astype(F32) * columns[0:CAP, t : t + 1]
        )


def weigh(part, weight, rows, earlier=()):
    return pl.pallas_call(
        weigh_kernel,
        grid=(PART,),
        in_specs=[
            pl.BlockSpec((OWN, TOK), lambda g: (part * PART + g, 0)),
            pl.BlockSpec((OWN, CAP, TOK), lambda g: (0, g, 0)),
        ]
        + [pl.BlockSpec(memory_space=pl.ANY)] * len(earlier),
        out_specs=pl.BlockSpec((OWN * CAP, TOK), lambda g: (part * PART + g, 0)),
        out_shape=shape((LISTS * CAP, TOK), F32),
        input_output_aliases={2: 0} if earlier else {},
        compiler_params=WIDE_PARAMS,
        name="weigh",
    )(weight, rows, *earlier)


def scatter_kernel(row_ref, wide_ref, out_ref, sq_ref, even_ref, odd_ref, come, go, *accs):
    step = pl.program_id(0)
    tables = (even_ref, odd_ref)

    def fetch(which, block):
        at = pl.multiple_of((block * 2 + which) * OWN, OWN)
        return pltpu.make_async_copy(
            row_ref.at[pl.ds(at, OWN), :], tables[which], come.at[which]
        )

    @pl.when(step == 0)
    def _():
        fetch(0, step).start()
        fetch(1, step).start()

        def clear(i, carry):
            at = pl.multiple_of(i * 64, 64)
            for acc in accs:
                acc[pl.ds(at, 64), :] = jnp.zeros((64, TOK), F32)
            return carry

        lax.fori_loop(0, ROWS // 64, clear, 0)

    for which in range(2):
        fetch(which, step).wait()
        waiting = []
        for t in range(OWN):
            for b in range(0, CAP, BATCH):
                made = []
                for j in range(b, b + BATCH):
                    acc = accs[j % ACCS]
                    row = tables[which][t, j]
                    at = (which * OWN + t) * CAP + j
                    made.append((acc, row, acc[pl.ds(row, 1), :] + wide_ref[at : at + 1, :]))
                for acc, row, total in waiting:
                    acc[pl.ds(row, 1), :] = total
                waiting = made
        for acc, row, total in waiting:
            acc[pl.ds(row, 1), :] = total

        @pl.when(step < pl.num_programs(0) - 1)
        def _():
            fetch(which, step + 1).start()

    @pl.when(step == pl.num_programs(0) - 1)
    def _():
        size = ROWS // CHUNKS
        sum_ref = accs[0]
        square_sum = jnp.zeros((8, TOK), F32)
        writes = []
        for c in range(CHUNKS):

            def collect(i, total):
                at = pl.multiple_of(c * size + i * 64, 64)
                value = sum_ref[pl.ds(at, 64), :]
                for acc in accs[1:]:
                    value = value + acc[pl.ds(at, 64), :]
                sum_ref[pl.ds(at, 64), :] = value
                square = value * value
                return total + jnp.sum(square.reshape(8, 8, TOK), axis=0)

            square_sum = lax.fori_loop(0, size // 64, collect, square_sum)
            part = pl.ds(c * size, size)
            writes.append(pltpu.make_async_copy(sum_ref.at[part, :], out_ref.at[part, :], go.at[c]))
            writes[c].start()
        sq_ref[...] = square_sum
        for write in writes:
            write.wait()


def scatter_rows(row, wide):
    return pl.pallas_call(
        scatter_kernel,
        grid=(NDP // 2,),
        in_specs=[
            pl.BlockSpec(memory_space=pltpu.HBM),
            pl.BlockSpec((2 * OWN * CAP, TOK), lambda g: (g, 0)),
        ],
        out_specs=[pl.BlockSpec(memory_space=pl.ANY)] + vmem(1),
        out_shape=(shape((ROWS, TOK), F32), shape((8, TOK), F32)),
        scratch_shapes=[
            pltpu.SMEM((OWN, TOK), jnp.int32),
            pltpu.SMEM((OWN, TOK), jnp.int32),
            pltpu.SemaphoreType.DMA((2,)),
            pltpu.SemaphoreType.DMA((CHUNKS,)),
        ]
        + [pltpu.VMEM((ROWS, TOK), F32) for _ in range(ACCS)],
        compiler_params=WIDE_PARAMS,
        name="scatter_rows",
    )(row, wide)


def finish_kernel(pieces_ref, sq_ref, part_ref, local_ref):
    part = pieces_ref[0]
    for t in range(1, OWN):
        part = part + pieces_ref[t]
    part_ref[...] = part
    square = part * part
    total = sq_ref[...] + (square[:, 0:TOK] + square[:, TOK:])
    total = jnp.sum(jnp.sum(total, axis=0, keepdims=True), axis=1, keepdims=True)
    local_ref[...] = jnp.broadcast_to(total, (1, TOK))


def finish(key_pieces, value_sq):
    return pl.pallas_call(
        finish_kernel,
        in_specs=vmem(2),
        out_specs=vmem(2),
        out_shape=(shape((8, HALF), F32), shape((1, TOK), F32)),
        compiler_params=PARAMS,
        name="finish",
    )(key_pieces, value_sq)


def scale_kernel(limit, sums_ref, part_ref, value_ref, out_ref, key_ref, clip_ref, buf, come, go):
    size = ROWS // CHUNKS

    def part_of(ref, i):
        return ref.at[pl.ds(i * size, size), :]

    reads = [
        pltpu.make_async_copy(part_of(value_ref, i), part_of(buf, i), come.at[i])
        for i in range(CHUNKS)
    ]
    writes = [
        pltpu.make_async_copy(part_of(buf, i), part_of(out_ref, i), go.at[i])
        for i in range(CHUNKS)
    ]
    for read in reads:
        read.start()
    total = jnp.sum(sums_ref[...], axis=0, keepdims=True)
    factor = jnp.minimum(1.0, limit / jnp.sqrt(total))
    clip_ref[...] = factor
    keys = part_ref[...] * jnp.concatenate([factor, factor], axis=1)
    for half in range(2):
        for head in range(2):
            r = half * 4 + head * 2
            key_ref[half, head] = keys[r : r + 2, :]
    for i in range(CHUNKS):
        reads[i].wait()
        at = slice(i * size, (i + 1) * size)
        buf[at, :] = buf[at, :] * factor
        writes[i].start()
    for write in writes:
        write.wait()


def scaled(limit, sums, key_part, value):
    return pl.pallas_call(
        functools.partial(scale_kernel, limit),
        in_specs=vmem(2) + [pl.BlockSpec(memory_space=pl.ANY)],
        out_specs=[pl.BlockSpec(memory_space=pl.ANY)] + vmem(2),
        out_shape=(
            shape((ROWS, TOK), F32),
            shape((2, 2, 2, HALF), F32),
            shape((1, TOK), F32),
        ),
        scratch_shapes=[
            pltpu.VMEM((ROWS, TOK), F32),
            pltpu.SemaphoreType.DMA((CHUNKS,)),
            pltpu.SemaphoreType.DMA((CHUNKS,)),
        ],
        compiler_params=WIDE_PARAMS,
        name="scale",
    )(sums, key_part, value)


def dscore_kernel(me_ref, ret_ref, *refs):
    late_refs = refs[:NDP]
    out_ref = refs[NDP]
    owner_id = lax.broadcasted_iota(jnp.int32, (OWN, TOK), 0)
    place_id = lax.broadcasted_iota(jnp.int32, (CAP, TOK), 0)
    row = lax.broadcasted_iota(jnp.int32, (PICKS, TOK), 0)
    for s in range(NDP):
        late_ref = late_refs[s]
        which = source(me_ref[0], s)
        square = jnp.concatenate([ret_ref[:, which, :]] * 4, axis=0)
        columns = jnp.transpose(square)[0:CAP, 0:OWN]
        stacked = jnp.concatenate(pieces(columns), axis=0)
        target = [late_index(late_ref, k, 3) for k in range(PICKS)]
        chosen = jnp.concatenate(
            [
                jnp.where(owner_id == jnp.right_shift(target[k], 7), 1.0, 0.0).astype(BF16)
                for k in range(PICKS)
            ],
            axis=1,
        )
        got = lax.dot_general(stacked, chosen, NN, preferred_element_type=F32)
        got = (got[0:CAP, :] + got[CAP : 2 * CAP, :]) + got[2 * CAP : 3 * CAP, :]
        picked = jnp.concatenate(
            [
                jnp.sum(
                    jnp.where(
                        place_id == jnp.bitwise_and(target[k], TOK - 1),
                        got[:, k * TOK : (k + 1) * TOK],
                        0.0,
                    ),
                    axis=0,
                    keepdims=True,
                )
                for k in range(PICKS)
            ],
            axis=0,
        )
        weight = jnp.concatenate(
            [
                joined(*[late_ref[p : p + 1, k * TOK : (k + 1) * TOK] for p in range(3)])
                for k in range(PICKS)
            ],
            axis=0,
        )
        both = weight * picked
        mean0 = jnp.sum(both[0:4, :], axis=0, keepdims=True)
        mean1 = jnp.sum(both[4:8, :], axis=0, keepdims=True)
        at = pl.multiple_of(which * 8, 8)
        slope = weight * (picked - jnp.where(row < 4, mean0, mean1))
        for d in range(NDP):
            out_ref[d, pl.ds(at, 8), :] = slope


def partial_dscore(me, returned, late):
    return pl.pallas_call(
        dscore_kernel,
        grid=(1,),
        in_specs=smem()
        + vmem(1)
        + [pl.BlockSpec((EXTRA, 4 * HALF), lambda g: (TOK // EXTRA, 0))] * NDP,
        out_specs=vmem(1)[0],
        out_shape=shape((NDP, NDP * PICKS, TOK), F32),
        compiler_params=PARAMS,
        name="dscore",
    )(me, returned, *late)


def key_kernel(me_ref, ds_ref, *refs):
    late_refs = refs[:NDP]
    out_ref = refs[NDP]
    base = me_ref[0] * KEYS
    dscore = []
    for s in range(NDP):
        at = pl.multiple_of(source(me_ref[0], s) * 8, 8)
        total = ds_ref[0, pl.ds(at, 8), :]
        for d in range(1, NDP):
            total = total + ds_ref[d, pl.ds(at, 8), :]
        dscore.append(total)
    key_id = lax.broadcasted_iota(jnp.int32, (KEYS, TOK), 0) + base
    for half in range(2):
        for head in range(2):
            at = head * 2 * HALF + half * HALF
            blocks = []
            for s in range(NDP):
                block = jnp.zeros((KEYS, TOK), F32)
                for k in range(4):
                    slot = head * 4 + k
                    value = dscore[s][slot : slot + 1, :]
                    block = block + jnp.where(
                        key_id == late_index(late_refs[s], slot, TOK + 5 + 2 * half), value, 0.0
                    )
                blocks.append(block)
            weighted = jnp.concatenate(blocks, axis=1)
            query = jnp.concatenate(
                [late_refs[s][0:TOK, at : at + HALF] for s in range(NDP)], axis=0
            )
            stacked = jnp.concatenate(pieces(weighted), axis=0)
            total = lax.dot_general(stacked, query, NN, preferred_element_type=F32)
            total = (total[0:KEYS, :] + total[KEYS : 2 * KEYS, :]) + total[2 * KEYS : 3 * KEYS, :]
            r = half * 4 + head * 2
            out_ref[:, r : r + 2, :] = total.reshape(OWN, 2, HALF)


def key_terms(me, dscore, late):
    return pl.pallas_call(
        key_kernel,
        in_specs=smem() + vmem(1 + NDP),
        out_specs=vmem(1)[0],
        out_shape=shape((OWN, 8, HALF), F32),
        compiler_params=PARAMS,
        name="key_terms",
    )(me, dscore, *late)


def exchange(x, axis):
    return lax.all_to_all(x, axis, 0, 0, tiled=True)


def everyone(x, axis, size):
    return exchange(jnp.broadcast_to(x[None], (size, *x.shape)), axis)


def body(queries, sub_keys, values, slot_first, slot_second, cotangent):
    q = queries.reshape(TOK, 4 * HALF)
    first = slot_first.reshape(TOK, PICKS).T
    second = slot_second.reshape(TOK, PICKS).T
    me = lax.axis_index("dp").astype(jnp.int32).reshape(1)
    outgoing, late = prep(q, sub_keys, first, second, cotangent)
    sent = exchange(outgoing, "dp")
    expanded = expand(0, sent)
    rows_a = exchange(expanded, TABLE)
    expanded = expand(1, sent)
    rows_b = exchange(expanded, TABLE)
    late, _ = lax.optimization_barrier((late, sent))
    late_all = [late] + [
        lax.ppermute(late, "dp", [(i, (i + k) % NDP) for i in range(NDP)])
        for k in range(1, NDP)
    ]
    row, weight = decode(rows_a)
    value_rows = gather_rows(row, values.reshape(ROWS, TOK))
    partial = dots(0, rows_a, value_rows)
    partial = dots(1, rows_b, value_rows, (partial,))
    returned = exchange(partial.reshape(OWN, NDP, TOK), TABLE)
    wide = weigh(0, weight, rows_a)
    wide = weigh(1, weight, rows_b, (wide,))
    value_grad, value_sq = scatter_rows(row, wide)
    slopes = partial_dscore(me, returned, late_all)
    dscore = exchange(slopes, "dp")
    key_grad = key_terms(me, dscore, late_all)
    key_pieces = exchange(key_grad, TABLE)
    key_part, local_sq = finish(key_pieces, value_sq)
    chip_sq = local_sq + lax.ppermute(local_sq, "table_2", [(0, 1), (1, 0)])
    sums = everyone(chip_sq, CHIPS, OWN * NDP // 2)
    limit = LIMIT_RATIO * math.sqrt(TOK * OWN * NDP)
    value_update, key_update, clip = scaled(
        limit, sums.reshape(OWN * NDP // 2, TOK), key_part, value_grad
    )
    return (
        value_update.reshape(BLK, NSUB, TOK),
        key_update,
        clip[0, 0:1],
    )


def solution(mesh):
    torus = Mesh(
        mesh.devices.reshape(mesh.shape["dp"], 4, 4, 2), ("dp", "table_0", "table_1", "table_2")
    )
    return jax.shard_map(
        body,
        mesh=torus,
        in_specs=(
            P(DP_TABLE, None, None),
            P(),
            P(TABLE, None, "dp"),
            P(DP_TABLE, None, None),
            P(DP_TABLE, None, None),
            P(DP_TABLE, None),
        ),
        out_specs=(P(TABLE, None, "dp"), P(None, None, DP_TABLE, None), P()),
        check_vma=False,
    )
```
